32 devices in a mesh: dp: 32 (over z, y, x, core).
Axes of the slice: x: 2, y: 2, z: 4, core: 2. Of those that a mesh axis runs over, the one named last changes fastest.
Arguments:
- tokens: bfloat16 [32768, 768], P('dp'), may hold values from -6 to 6
- cotangent: bfloat16 [32768, 768], P('dp'), may hold values from -6 to 6
- lengths: int32 [64], P('dp'), may hold values from 128 to 512, as said below
- counts: int32 [32], P('dp'), may hold values from 1 to 2, as said below
- attn_w: float32 [2, 768, 3072], P(None, 'dp')
- ffn_w: float32 [2, 768, 6144], P(None, 'dp')
- vec_w: float32 [2, 12, 768], P(None, None, 'dp')
- attn_m: float32 [2, 768, 3072], P(None, 'dp'), may hold values from -3 to 3
- ffn_m: float32 [2, 768, 6144], P(None, 'dp'), may hold values from -3 to 3
- vec_m: float32 [2, 12, 768], P(None, None, 'dp'), may hold values from -3 to 3
- attn_v: float32 [2, 768, 3072], P(None, 'dp'), may hold values from 0.001 to 0.1
- ffn_v: float32 [2, 768, 6144], P(None, 'dp'), may hold values from 0.001 to 0.1
- vec_v: float32 [2, 12, 768], P(None, None, 'dp'), may hold values from 0.001 to 0.1
Outputs:
- activations: bfloat16 [32768, 768], P('dp')
- in_grad: float32 [32768, 768], P('dp')
- attn_grad: float32 [2, 768, 3072], P(None, 'dp')
- ffn_grad: float32 [2, 768, 6144], P(None, 'dp')
- vec_grad: float32 [2, 12, 768], P(None, None, 'dp')
- attn_step: float32 [2, 768, 3072], P(None, 'dp')
- ffn_step: float32 [2, 768, 6144], P(None, 'dp')
- vec_step: float32 [2, 12, 768], P(None, None, 'dp')
- attn_m_new: float32 [2, 768, 3072], P(None, 'dp')
- ffn_m_new: float32 [2, 768, 6144], P(None, 'dp')
- vec_m_new: float32 [2, 12, 768], P(None, None, 'dp')
- attn_v_new: float32 [2, 768, 3072], P(None, 'dp')
- ffn_v_new: float32 [2, 768, 6144], P(None, 'dp')
- vec_v_new: float32 [2, 12, 768], P(None, None, 'dp')
The draws below stay inside these ranges and needn't reach their ends.
Inputs may be any that keep to these rules, and one draw needn't show every extreme that they name: `lengths`: some sequence has exactly 512 valid tokens. `counts`: some group has exactly 2 live microbatches.
All inputs are finite; a program needn't handle non-finite values.
Results may differ from the reference program's by a relative error of at most 0.02.
Values may be sent and summed in bfloat16 or wider, within the bound.
A program may use at most 320 MiB of HBM per device.

```python
import math
import jax
import jax.numpy as jnp
from jax import lax

D = 768
HEADS = 12
HEAD_DIM = 64
FF = 3072
SEQ = 512
LAYERS = 2
MB_DEV = 2
SEQ_MB = 1
SEQ_DEV = 2
SEQS = 64
TOKENS = 32768
GROUPS = 32
VROWS = 12


def draw_lengths(key, part):
    drawn = jax.random.randint(key, (SEQS,), SEQ // 4, SEQ + 1)
    place = jax.random.randint(jax.random.fold_in(key, 11), (), 0, SEQS)
    return drawn.at[place].set(SEQ).astype(jnp.int32)


def draw_counts(key, part):
    picked = jax.random.randint(key, (GROUPS,), 0, 8)
    drawn = jnp.where(picked == 0, MB_DEV, 1)
    place = jax.random.randint(jax.random.fold_in(key, 13), (), 0, GROUPS)
    return drawn.at[place].set(MB_DEV).astype(jnp.int32)


def draw_attn_w(key, part):
    normal = jax.random.normal(key, (LAYERS, D, 4 * D), jnp.float32)
    column = lax.broadcasted_iota(jnp.int32, (LAYERS, D, 4 * D), 2)
    factor = jnp.where(column >= 3 * D, 8.0, 1.0)
    return normal * factor * D ** (-0.5)


def draw_ffn_w(key, part):
    normal = jax.random.normal(key, (LAYERS, D, 2 * FF), jnp.float32)
    column = lax.broadcasted_iota(jnp.int32, (LAYERS, D, 2 * FF), 2)
    factor = jnp.where(column < FF, D ** (-0.5), FF ** (-0.5))
    return normal * factor


def draw_vec_w(key, part):
    normal = jax.random.normal(key, (LAYERS, VROWS, D), jnp.float32) * 0.2
    rowpos = lax.broadcasted_iota(jnp.int32, (LAYERS, VROWS, D), 1)
    offset = jnp.where((rowpos == 3) | (rowpos == 5), 1.0, 0.0)
    return normal + offset


def spiked(values, key, source, target, shards_of, factor):
    def block_of(position):
        return (jnp.arange(values.shape[position]) // (values.shape[position] // shards_of)).reshape((-1,) + (1,) * (values.ndim - 1 - position))

    one_side = jax.random.permutation(key, shards_of)[block_of(target)]
    second = (block_of(target) + shards_of // 2) % shards_of
    return jnp.where((block_of(source) == one_side) | (block_of(source) == second), factor * values, values)


def steps_of(stream_key, extent, pieces, least, top_value):
    level, own = 1.0, jax.random.fold_in(stream_key, 6)
    for dim, parts in pieces:
        steps = jnp.exp(jax.random.uniform(jax.random.fold_in(own, dim), (parts,), jnp.float32, least / len(pieces), top_value / len(pieces)))
        level = level * jnp.repeat(steps, extent[dim] // parts).reshape([-1 if axis == dim else 1 for axis in range(len(extent))])
    return level


def bell_draw(own_key, dims, deviation, limit, shards=(), held_as=jnp.bfloat16):
    result = deviation * jax.random.normal(own_key, dims, jnp.float32)
    if shards:
        result = result * steps_of(own_key, dims, shards, -0.22, 0.18)
    return jnp.clip(result, -limit, limit).astype(held_as)


def gaussian_with(stream_key, dims, width, limit, cuts, heavy, held_as=jnp.bfloat16):
    values = width * jax.random.normal(stream_key, dims, jnp.float32)
    if cuts:
        values = values * steps_of(stream_key, dims, cuts, -0.22, 0.18)
    return jnp.clip(spiked(values, jax.random.fold_in(stream_key, 3), *heavy), -limit, limit).astype(held_as)


def setup_inputs(seed: int = 0) -> dict:
    arg_keys = jax.random.split(jax.random.key(seed), 14)
    return {
        "tokens": bell_draw(arg_keys[0], (TOKENS, D), 1.0, 6.0, ((0, 32),)),
        "cotangent": gaussian_with(arg_keys[1], (TOKENS, D), 1.0, 6.0, ((0, 32),), (0, 1, 32, 2.75)),
        "lengths": draw_lengths(jax.random.fold_in(arg_keys[13], 71), 0),
        "counts": draw_counts(jax.random.fold_in(arg_keys[13], 71), 0),
        "attn_w": draw_attn_w(jax.random.fold_in(arg_keys[13], 71), 0),
        "ffn_w": draw_ffn_w(jax.random.fold_in(arg_keys[13], 71), 0),
        "vec_w": draw_vec_w(jax.random.fold_in(arg_keys[13], 71), 0),
        "attn_m": bell_draw(arg_keys[7], (LAYERS, D, 4 * D), 0.3, 3.0, ((1, 32),), jnp.float32),
        "ffn_m": bell_draw(arg_keys[8], (LAYERS, D, 2 * FF), 0.3, 3.0, ((1, 32),), jnp.float32),
        "vec_m": bell_draw(arg_keys[9], (LAYERS, VROWS, D), 0.3, 3.0, ((2, 32),), jnp.float32),
        "attn_v": jnp.clip(jnp.exp(math.log(0.1) - 4.6051702 * jax.random.uniform(arg_keys[10], (LAYERS, D, 4 * D), jnp.float32) ** steps_of(arg_keys[10], (LAYERS, D, 4 * D), ((1, 32),), -0.2, 0.2)), 0.001, 0.1),
        "ffn_v": jnp.clip(jnp.exp(math.log(0.1) - 4.6051702 * jax.random.uniform(arg_keys[11], (LAYERS, D, 2 * FF), jnp.float32) ** steps_of(arg_keys[11], (LAYERS, D, 2 * FF), ((1, 32),), -0.2, 0.2)), 0.001, 0.1),
        "vec_v": jnp.clip(jnp.exp(math.log(0.1) - 4.6051702 * jax.random.uniform(arg_keys[12], (LAYERS, VROWS, D), jnp.float32) ** steps_of(arg_keys[12], (LAYERS, VROWS, D), ((2, 32),), -0.2, 0.2)), 0.001, 0.1),
    }


@jax.custom_vjp
def low(v):
    return lax.optimization_barrier(v.astype(jnp.bfloat16)).astype(jnp.float32)

@jax.custom_vjp
def low_back(v):
    return v

def low_keep(v):
    return (low(v), None)

def low_pass(kept, grad):
    return (grad,)

def back_keep(v):
    return (v, None)

def back_low(kept, grad):
    return (low(grad),)
low.defvjp(low_keep, low_pass)
low_back.defvjp(back_keep, back_low)
NORM_EPS = 1e-05
MASK_VALUE = -1e+30

def layer_norm(value, gain, shift):
    centred = value - lax.optimization_barrier(jnp.mean(value, axis=-1, keepdims=True))
    inverse = lax.rsqrt(lax.optimization_barrier(jnp.mean(centred * centred, axis=-1, keepdims=True)) + NORM_EPS)
    return centred * inverse * gain + shift

def matmul(left, right):
    return jnp.dot(left, right, precision=lax.Precision.HIGHEST)

def layer_forward(rows, attn, ffn, vector, valid):
    attn = low(attn)
    ffn = low(ffn)
    vector = low(vector)
    seq_count = valid.shape[0]

    def heads(value):
        return value.reshape(seq_count, SEQ, HEADS, HEAD_DIM)
    query = low_back(low(matmul(rows, attn[:, :D]) + vector[0]))
    keys = low_back(low(matmul(rows, attn[:, D:2 * D])))
    values = low_back(low(matmul(rows, attn[:, 2 * D:3 * D]) + vector[1]))
    scores = jnp.einsum('sqhe,skhe->shqk', heads(query), heads(keys), precision=lax.Precision.HIGHEST)
    scores = low_back(scores * HEAD_DIM ** (-0.5))
    scores = jnp.where(valid[:, None, None, :], scores, MASK_VALUE)
    chances = low(jax.nn.softmax(scores, axis=-1))
    context = jnp.einsum('shqk,skhe->sqhe', chances, heads(values), precision=lax.Precision.HIGHEST)
    context = low_back(low(context.reshape(rows.shape[0], D)))
    attn_out = low_back(matmul(context, attn[:, 3 * D:].T) + vector[2])
    normed = low(layer_norm(rows + attn_out, vector[3], vector[4]))
    inner = low_back(matmul(normed, ffn[:, :FF]) + vector[8:].reshape(FF))
    active = low(jax.nn.gelu(inner, approximate=False))
    ffn_out = low_back(matmul(active, ffn[:, FF:].T) + vector[7])
    return low(layer_norm(normed + ffn_out, vector[5], vector[6]))

def adam_step(param, first, second, grad):
    first_new = 0.9 * first + 0.1 * grad
    second_new = 0.98 * second + 0.02 * grad * grad
    first_hat = first_new / (1.0 - 0.9 ** 10)
    second_hat = second_new / (1.0 - 0.98 ** 10)
    direction = first_hat / (jnp.sqrt(second_hat) + 1e-08) + 0.01 * param
    return (direction, first_new, second_new)

def reference(tokens, cotangent, lengths, counts, attn_w, ffn_w, vec_w, attn_m, ffn_m, vec_m, attn_v, ffn_v, vec_v):
    seq_total = lengths.shape[0]
    group = math.gcd(seq_total, 8)
    blocks = seq_total // group
    seq_index = jnp.arange(seq_total, dtype=jnp.int32)
    owner = seq_index // SEQ_DEV
    micro = seq_index % SEQ_DEV // SEQ_MB
    live = (micro < jnp.take(counts, owner)).astype(jnp.float32)
    valid = jnp.arange(SEQ, dtype=jnp.int32)[None, :] < lengths[:, None]
    inputs = tokens.astype(jnp.float32).reshape(blocks, group, SEQ, D)
    masked_cot = cotangent.astype(jnp.float32).reshape(seq_total, SEQ, D) * live[:, None, None]
    masked_cot = masked_cot.reshape(blocks, group, SEQ, D)
    valid_blocks = valid.reshape(blocks, group, SEQ)
    params = (attn_w, ffn_w, vec_w)

    def one_block(totals, items):
        block_in, block_cot, block_valid = items

        def model(weights, block_rows):
            rows = block_rows.reshape(group * SEQ, D)
            for layer in range(LAYERS):
                rows = layer_forward(rows, weights[0][layer], weights[1][layer], weights[2][layer], block_valid)
            return rows
        output, pull = jax.vjp(model, params, block_in)
        grads, grad_in = pull(block_cot.reshape(group * SEQ, D))
        totals = jax.tree.map(jnp.add, totals, grads)
        return (totals, (output, grad_in))
    zeros = jax.tree.map(jnp.zeros_like, params)
    totals, (outputs, grads_in) = lax.scan(one_block, zeros, (inputs, masked_cot, valid_blocks))
    activations = (outputs.reshape(seq_total, SEQ, D) * live[:, None, None]).reshape(TOKENS, D).astype(jnp.bfloat16)
    in_grad = grads_in.reshape(TOKENS, D)
    factor = float(TOKENS) ** (-0.5)
    attn_grad = totals[0] * factor
    ffn_grad = totals[1] * factor
    vec_grad = totals[2] * factor
    attn_step, attn_m_new, attn_v_new = adam_step(attn_w, attn_m, attn_v, attn_grad)
    ffn_step, ffn_m_new, ffn_v_new = adam_step(ffn_w, ffn_m, ffn_v, ffn_grad)
    vec_step, vec_m_new, vec_v_new = adam_step(vec_w, vec_m, vec_v, vec_grad)
    return (activations, in_grad, attn_grad, ffn_grad, vec_grad, attn_step, ffn_step, vec_step, attn_m_new, ffn_m_new, vec_m_new, attn_v_new, ffn_v_new, vec_v_new)
```

```python
import functools

import jax
import jax.numpy as jnp
from jax import lax
from jax.experimental import pallas as pl
from jax.experimental.pallas import tpu as pltpu
from jax.sharding import PartitionSpec as P

HEAD_DIM = 64
SEQ_MB = 1
PAIR = 2 * HEAD_DIM

NORM_EPS = 1e-05
MASK_VALUE = -1e30

TAIL_P = 0.275
TAIL_C = (0.1178092576, 0.04211145346, 0.3339323636, -0.3309935012, 0.4519987806, -0.1148583494)
INV_SQRT_2PI = 0.3989422804014327


def lowered(value):
    return value.astype(jnp.bfloat16)


def project(left, right):
    return jnp.dot(left, right, preferred_element_type=jnp.float32)


def project_back(left, right):
    return lax.dot_general(
        left, right, (((1,), (1,)), ((), ())), preferred_element_type=jnp.float32
    )


def outer_sum(left, right):
    return lax.dot_general(
        left, right, (((0,), (0,)), ((), ())), preferred_element_type=jnp.float32
    )


def bit_count(devices):
    bits = devices.bit_length() - 1
    assert 1 << bits == devices
    return bits


def swap(value, bit):
    devices = lax.axis_size("dp")
    return lax.ppermute(value, "dp", [(i, i ^ (1 << bit)) for i in range(devices)])


def gather_rows(shard, flip):
    bits = bit_count(lax.axis_size("dp"))
    rows = shard
    for bit in reversed(range(3 if flip else 0, bits)):
        rows = jnp.concatenate([rows, swap(rows, bit)], axis=0)
    if flip:
        height, width = rows.shape
        rows = jnp.concatenate([rows[None], swap(rows, 1)[None]], axis=0)
        rows = jnp.concatenate([rows[:, None], swap(rows, 2)[:, None]], axis=1)
        rows = rows.reshape(4 * height, width)
        rows = jnp.concatenate([rows, swap(rows, 0)], axis=0)
    return rows


def scatter_rows(keep, send, flip, wire):
    bits = bit_count(lax.axis_size("dp"))
    total = keep + swap(send.astype(wire), 0).astype(jnp.float32)
    start = 1
    if flip:
        total = total.astype(wire)
        height, width = total.shape
        quarter = total.reshape(2, 2, height // 4, width)
        total = quarter[:, 0].astype(jnp.float32) + swap(quarter[:, 1], 2).astype(jnp.float32)
        total = total.astype(wire)
        total = total[0].astype(jnp.float32) + swap(total[1], 1).astype(jnp.float32)
        start = 3
    for bit in range(start, bits):
        total = total.astype(wire)
        half = total.shape[0] // 2
        total = total[:half].astype(jnp.float32) + swap(total[half:], bit).astype(jnp.float32)
    return total


def outer_scatter(left, right, flip):
    half = left.shape[1] // 2
    send = lowered(outer_sum(left[:, half:], right))
    keep = outer_sum(left[:, :half], right)
    return scatter_rows(keep, send, flip, jnp.bfloat16)


def order_matrix(width):
    devices = lax.axis_size("dp")
    bits = bit_count(devices)
    block = width // devices
    place = lax.broadcasted_iota(jnp.int32, (width, width), 1)
    feature = lax.broadcasted_iota(jnp.int32, (width, width), 0)
    part = place // block
    mirrored = jnp.zeros_like(part)
    for bit in range(bits):
        mirrored = mirrored | (((part >> bit) & 1) << (bits - 1 - bit))
    wanted = (mirrored ^ lax.axis_index("dp")) * block + place % block
    return (feature == wanted).astype(jnp.bfloat16)


def head_lanes(which):
    return lax.broadcasted_iota(jnp.int32, (1, PAIR), 1) // HEAD_DIM == which


def attend_kernel(len_ref, q_ref, k_ref, v_ref, ctx_ref):
    length = len_ref[pl.program_id(0)]
    seq = k_ref.shape[0]
    query = q_ref[...] * jnp.bfloat16(HEAD_DIM ** (-0.5))
    keys = k_ref[...]
    values = v_ref[...]
    open_keys = lax.broadcasted_iota(jnp.int32, (1, seq), 1) < length
    picked = []
    for which in range(2):
        lanes = head_lanes(which)
        scores = project_back(jnp.where(lanes, query, jnp.zeros_like(query)), keys)
        scores = jnp.where(open_keys, scores, MASK_VALUE)
        expo = jnp.exp(scores - jnp.max(scores, axis=-1, keepdims=True))
        chance = expo * (1.0 / jnp.sum(expo, axis=-1, keepdims=True))
        picked.append(project(lowered(chance), values))
    ctx_ref[...] = lowered(jnp.where(head_lanes(0), picked[0], picked[1]))


def attend(lengths, qk, values, seq):
    rows, width = values.shape
    pairs = width // PAIR
    flops = 4 * rows * seq * width
    return pl.pallas_call(
        attend_kernel,
        grid_spec=pltpu.PrefetchScalarGridSpec(
            num_scalar_prefetch=1,
            grid=(rows // seq, pairs),
            in_specs=[
                pl.BlockSpec((seq, PAIR), lambda s, h, n: (s, h)),
                pl.BlockSpec((seq, PAIR), lambda s, h, n: (s, pairs + h)),
                pl.BlockSpec((seq, PAIR), lambda s, h, n: (s, h)),
            ],
            out_specs=pl.BlockSpec((seq, PAIR), lambda s, h, n: (s, h)),
        ),
        out_shape=jax.ShapeDtypeStruct((rows, width), jnp.bfloat16),
        cost_estimate=pl.CostEstimate(
            flops=8 * flops, bytes_accessed=8 * rows * width, transcendentals=rows * seq * 12
        ),
        name="attend",
    )(lengths, qk, qk, values)


def attend_back_kernel(len_ref, q_ref, k_ref, v_ref, g_ref, dq_ref, dk_ref, dv_ref):
    length = len_ref[pl.program_id(0)]
    seq = k_ref.shape[0]
    query = q_ref[...] * jnp.bfloat16(HEAD_DIM ** (-0.5))
    keys = k_ref[...]
    values = v_ref[...]
    grads = g_ref[...]
    open_keys = lax.broadcasted_iota(jnp.int32, (seq, 1), 0) < length
    parts = []
    for which in range(2):
        lanes = head_lanes(which)
        scores = project_back(keys, jnp.where(lanes, query, jnp.zeros_like(query)))
        scores = jnp.where(open_keys, scores, MASK_VALUE)
        expo = jnp.exp(scores - jnp.max(scores, axis=0, keepdims=True))
        chance = expo * (1.0 / jnp.sum(expo, axis=0, keepdims=True))
        grad_chance = project_back(values, jnp.where(lanes, grads, jnp.zeros_like(grads)))
        weighed = jnp.sum(chance * grad_chance, axis=0, keepdims=True)
        grad_scores = lowered(chance * (grad_chance - weighed))
        parts.append(
            (
                outer_sum(grad_scores, keys) * HEAD_DIM ** (-0.5),
                project(grad_scores, query),
                project(lowered(chance), grads),
            )
        )
    first = head_lanes(0)
    for index, out_ref in enumerate((dq_ref, dk_ref, dv_ref)):
        out_ref[...] = lowered(jnp.where(first, parts[0][index], parts[1][index]))


def attend_back(lengths, qk, values, grads, seq):
    rows, width = values.shape
    pairs = width // PAIR
    flops = 10 * rows * seq * width
    spec = pl.BlockSpec((seq, PAIR), lambda s, h, n: (s, h))
    shape = jax.ShapeDtypeStruct((rows, width), jnp.bfloat16)
    return pl.pallas_call(
        attend_back_kernel,
        grid_spec=pltpu.PrefetchScalarGridSpec(
            num_scalar_prefetch=1,
            grid=(rows // seq, pairs),
            in_specs=[
                spec,
                pl.BlockSpec((seq, PAIR), lambda s, h, n: (s, pairs + h)),
                spec,
                spec,
            ],
            out_specs=[spec, spec, spec],
        ),
        out_shape=[shape, shape, shape],
        cost_estimate=pl.CostEstimate(
            flops=8 * flops, bytes_accessed=14 * rows * width, transcendentals=rows * seq * 12
        ),
        name="attend_back",
    )(lengths, qk, qk, values, grads)


def expand_kernel(h_ref, w_ref, b_ref, u_ref, slope_ref):
    inner = project(h_ref[...], w_ref[...]) + b_ref[...]
    bell = jnp.exp(inner * inner * -0.5)
    step = 1.0 / (1.0 + TAIL_P * jnp.abs(inner))
    poly = jnp.full_like(step, TAIL_C[-1])
    for coefficient in reversed(TAIL_C[:-1]):
        poly = poly * step + coefficient
    tail = poly * step * bell
    below = jnp.where(inner >= 0, 1.0 - tail, tail)
    u_ref[...] = lowered(inner * below)
    slope_ref[...] = lowered(below + inner * bell * INV_SQRT_2PI)


def expand(normed, weight, bias, tile=256):
    rows, width = normed.shape
    hidden = weight.shape[1]
    shape = jax.ShapeDtypeStruct((rows, hidden), jnp.bfloat16)
    out_spec = pl.BlockSpec((rows, tile), lambda j: (0, j))
    return pl.pallas_call(
        expand_kernel,
        grid=(hidden // tile,),
        in_specs=[
            pl.BlockSpec((rows, width), lambda j: (0, 0)),
            pl.BlockSpec((width, tile), lambda j: (0, j)),
            pl.BlockSpec((1, tile), lambda j: (0, j)),
        ],
        out_specs=[out_spec, out_spec],
        out_shape=[shape, shape],
        cost_estimate=pl.CostEstimate(
            flops=6 * rows * width * hidden,
            bytes_accessed=2 * width * hidden + 4 * rows * hidden,
            transcendentals=2 * rows * hidden,
        ),
        name="expand",
    )(normed, weight, bias)


def norm_parts(value):
    centred = value - jnp.mean(value, axis=-1, keepdims=True)
    inverse = lax.rsqrt(jnp.mean(centred * centred, axis=-1, keepdims=True) + NORM_EPS)
    return centred * inverse, inverse


def norm_back(grad, value, gain):
    unit, inverse = norm_parts(value)
    grad_gain = jnp.sum(grad * unit, axis=0)
    grad_shift = jnp.sum(grad, axis=0)
    grad_unit = grad * gain
    grad_value = inverse * (
        grad_unit
        - jnp.mean(grad_unit, axis=-1, keepdims=True)
        - unit * jnp.mean(grad_unit * unit, axis=-1, keepdims=True)
    )
    return grad_value, grad_gain, grad_shift


def layer_ahead(rows, weights, lengths, seq):
    w_qk, w_vo, w_up, w_down, vec_place, vec_plain = weights
    width = rows.shape[1]
    bias_q, bias_v, bias_up = vec_plain[0], vec_plain[1], vec_plain[8:12].reshape(1, -1)
    bias_qk = jnp.concatenate([bias_q, jnp.zeros_like(bias_q)])
    qk = lowered(project(rows, w_qk) + bias_qk)
    values = lowered(project(rows, w_vo[:, :width]) + bias_v)
    context = attend(lengths, qk, values, seq)
    first_sum = (
        rows.astype(jnp.float32) + project_back(context, w_vo[:, width : 2 * width]) + vec_place[2]
    )
    normed = lowered(norm_parts(first_sum)[0] * vec_place[3] + vec_place[4])
    active, slope = expand(normed, w_up, bias_up)
    second_sum = normed.astype(jnp.float32) + project_back(active, w_down) + vec_place[7]
    output = lowered(norm_parts(second_sum)[0] * vec_place[5] + vec_place[6])
    return output, (qk, values, context, first_sum, normed, active, slope, second_sum)


def layer_behind(grad_out, rows, kept, weights, lengths, seq, spread):
    w_qk, w_vo, w_up, w_down, vec_place, vec_plain = weights
    width = rows.shape[1]
    qk, values, context, first_sum, normed, active, slope, second_sum = kept
    grad_second, gain_two, shift_two = norm_back(grad_out, second_sum, vec_place[5])
    grad_ffn = lowered(grad_second)
    bias_out = jnp.sum(grad_ffn.astype(jnp.float32), axis=0)
    down_grad = outer_scatter(grad_ffn, active, True)
    grad_inner = lowered(project(grad_ffn, w_down) * slope.astype(jnp.float32))
    bias_inner = jnp.sum(grad_inner.astype(jnp.float32), axis=0)
    up_grad = outer_scatter(normed, grad_inner, False)
    grad_normed = grad_second + project_back(grad_inner, w_up)
    grad_first, gain_one, shift_one = norm_back(grad_normed, first_sum, vec_place[3])
    grad_attn = lowered(grad_first)
    bias_attn = jnp.sum(grad_attn.astype(jnp.float32), axis=0)
    out_grad = outer_scatter(grad_attn, context, True)
    grad_context = lowered(project(grad_attn, w_vo[:, width : 2 * width]))
    grad_query, grad_keys, grad_values = attend_back(lengths, qk, values, grad_context, seq)
    bias_query = jnp.sum(grad_query.astype(jnp.float32), axis=0)
    bias_value = jnp.sum(grad_values.astype(jnp.float32), axis=0)
    value_grad = outer_scatter(rows, grad_values, True)
    query_grad = outer_scatter(rows, grad_query, False)
    key_grad = outer_scatter(rows, grad_keys, False)
    grad_rows = grad_first + project_back(grad_query, w_qk[:, :width])
    grad_rows = grad_rows + project_back(grad_keys, w_qk[:, width:])
    grad_rows = grad_rows + project_back(grad_values, w_vo[:, :width])
    plain = jnp.concatenate(
        [jnp.stack([bias_query, bias_value]), bias_inner.reshape(-1, width)], axis=0
    )
    placed = jnp.dot(plain, spread.astype(jnp.float32), precision=lax.Precision.HIGHEST)
    vec_grad = jnp.stack(
        [
            placed[0],
            placed[1],
            bias_attn,
            gain_one,
            shift_one,
            gain_two,
            shift_two,
            bias_out,
            placed[2],
            placed[3],
            placed[4],
            placed[5],
        ],
        axis=1,
    )
    attn_grad = jnp.concatenate([query_grad, key_grad, value_grad, out_grad], axis=1)
    ffn_grad = jnp.concatenate([up_grad, down_grad], axis=1)
    return grad_rows, (attn_grad, ffn_grad, vec_grad)


def adam_step(param, first, second, grad):
    first_new = 0.9 * first + 0.1 * grad
    second_new = 0.98 * second + 0.02 * grad * grad
    first_hat = first_new / (1.0 - 0.9**10)
    second_hat = second_new / (1.0 - 0.98**10)
    direction = first_hat / (jnp.sqrt(second_hat) + 1e-08) + 0.01 * param
    return (direction, first_new, second_new)


def local(
    tokens,
    cotangent,
    lengths,
    counts,
    attn_w,
    ffn_w,
    vec_w,
    attn_m,
    ffn_m,
    vec_m,
    attn_v,
    ffn_v,
    vec_v,
):
    row_total, width = tokens.shape
    seq = row_total // lengths.shape[0]
    layers = attn_w.shape[0]
    hidden = ffn_w.shape[2] // 2
    vec_rows = vec_w.shape[1]
    micro = lax.broadcasted_iota(jnp.int32, (row_total, 1), 0) // (seq * SEQ_MB)
    live = micro < counts[0]
    spread = order_matrix(width)
    weights_all = []
    for layer in range(layers):
        attn = lowered(attn_w[layer])
        ffn = lowered(ffn_w[layer])
        vec = jnp.pad(jnp.transpose(lowered(vec_w[layer])), ((0, 0), (0, 128 - vec_rows)))
        w_qk = gather_rows(attn[:, : 2 * width], False)
        w_vo = gather_rows(jnp.concatenate([attn[:, 2 * width :], vec], axis=1), True)
        vec_place = w_vo[:, 2 * width :]
        vec_plain = jnp.transpose(project(spread, vec_place))
        vec_place = jnp.transpose(vec_place.astype(jnp.float32))
        w_up = gather_rows(ffn[:, :hidden], False)
        w_down = gather_rows(ffn[:, hidden:], True)
        weights_all.append((w_qk, w_vo, w_up, w_down, vec_place, vec_plain))
    rows = lowered(project(tokens, spread))
    kept_all = []
    layer_inputs = []
    for layer in range(layers):
        layer_inputs.append(rows)
        rows, kept = layer_ahead(rows, weights_all[layer], lengths, seq)
        kept_all.append(kept)
    activations = lowered(jnp.where(live, project_back(rows, spread), 0.0))
    grad_rows = jnp.where(live, project(cotangent, spread), 0.0)
    summed_all = [None] * layers
    for layer in reversed(range(layers)):
        grad_rows, summed_all[layer] = layer_behind(
            grad_rows,
            layer_inputs[layer],
            kept_all[layer],
            weights_all[layer],
            lengths,
            seq,
            spread,
        )
    high = lax.reduce_precision(grad_rows, 8, 7)
    in_grad = project_back(lowered(high), spread) + project_back(lowered(grad_rows - high), spread)
    vec_local = jnp.concatenate([summed_all[index][2] for index in range(layers)], axis=1)
    half = width // 2
    vec_sum = scatter_rows(vec_local[:half], vec_local[half:], False, jnp.float32)
    vec_sum = jnp.transpose(vec_sum).reshape(layers, vec_rows, -1)
    factor = float(row_total * lax.axis_size("dp")) ** (-0.5)
    attn_grad = jnp.stack([summed_all[index][0] for index in range(layers)]) * factor
    ffn_grad = jnp.stack([summed_all[index][1] for index in range(layers)]) * factor
    vec_grad = vec_sum * factor
    attn_step, attn_m_new, attn_v_new = adam_step(attn_w, attn_m, attn_v, attn_grad)
    ffn_step, ffn_m_new, ffn_v_new = adam_step(ffn_w, ffn_m, ffn_v, ffn_grad)
    vec_step, vec_m_new, vec_v_new = adam_step(vec_w, vec_m, vec_v, vec_grad)
    return (
        activations,
        in_grad,
        attn_grad,
        ffn_grad,
        vec_grad,
        attn_step,
        ffn_step,
        vec_step,
        attn_m_new,
        ffn_m_new,
        vec_m_new,
        attn_v_new,
        ffn_v_new,
        vec_v_new,
    )


def solution(mesh):
    rows = P("dp", None)
    weight = P(None, "dp", None)
    vector = P(None, None, "dp")
    in_specs = (rows, rows, P("dp"), P("dp")) + (weight, weight, vector) * 3
    out_specs = (rows, rows) + (weight, weight, vector) * 4
    return jax.shard_map(local, mesh=mesh, in_specs=in_specs, out_specs=out_specs, check_vma=False)
```

```python
import functools

import jax
import jax.numpy as jnp
from jax import lax
from jax.experimental import pallas as pl
from jax.experimental.pallas import tpu as pltpu
from jax.sharding import PartitionSpec as P

HEAD_DIM = 64
SEQ_MB = 1
PAIR = 2 * HEAD_DIM

NORM_EPS = 1e-05
MASK_VALUE = -1e30

TAIL_P = 0.275
TAIL_C = (0.1178092576, 0.04211145346, 0.3339323636, -0.3309935012, 0.4519987806, -0.1148583494)
INV_SQRT_2PI = 0.3989422804014327


def lowered(value):
    return value.astype(jnp.bfloat16)


def project(left, right):
    return jnp.dot(left, right, preferred_element_type=jnp.float32)


def project_back(left, right):
    return lax.dot_general(
        left, right, (((1,), (1,)), ((), ())), preferred_element_type=jnp.float32
    )


def outer_sum(left, right):
    return lax.dot_general(
        left, right, (((0,), (0,)), ((), ())), preferred_element_type=jnp.float32
    )


def bit_count(devices):
    bits = devices.bit_length() - 1
    assert 1 << bits == devices
    return bits


def swap(value, bit):
    devices = lax.axis_size("dp")
    return lax.ppermute(value, "dp", [(i, i ^ (1 << bit)) for i in range(devices)])


def gather_rows(shard, flip):
    bits = bit_count(lax.axis_size("dp"))
    rows = shard
    for bit in reversed(range(3 if flip else 0, bits)):
        rows = jnp.concatenate([rows, swap(rows, bit)], axis=0)
    if flip:
        height, width = rows.shape
        rows = jnp.concatenate([rows[None], swap(rows, 1)[None]], axis=0)
        rows = jnp.concatenate([rows[:, None], swap(rows, 2)[:, None]], axis=1)
        rows = rows.reshape(4 * height, width)
        rows = jnp.concatenate([rows, swap(rows, 0)], axis=0)
    return rows


def scatter_rows(keep, send, flip, wire):
    bits = bit_count(lax.axis_size("dp"))
    total = keep + swap(send.astype(wire), 0).astype(jnp.float32)
    start = 1
    if flip:
        total = total.astype(wire)
        height, width = total.shape
        quarter = total.reshape(2, 2, height // 4, width)
        total = quarter[:, 0].astype(jnp.float32) + swap(quarter[:, 1], 2).astype(jnp.float32)
        total = total.astype(wire)
        total = total[0].astype(jnp.float32) + swap(total[1], 1).astype(jnp.float32)
        start = 3
    for bit in range(start, bits):
        total = total.astype(wire)
        half = total.shape[0] // 2
        total = total[:half].astype(jnp.float32) + swap(total[half:], bit).astype(jnp.float32)
    return total


def outer_scatter(left, right, flip):
    half = left.shape[1] // 2
    send = lowered(outer_sum(left[:, half:], right))
    keep = outer_sum(left[:, :half], right)
    return scatter_rows(keep, send, flip, jnp.bfloat16)


def order_matrix(width):
    devices = lax.axis_size("dp")
    bits = bit_count(devices)
    block = width // devices
    place = lax.broadcasted_iota(jnp.int32, (width, width), 1)
    feature = lax.broadcasted_iota(jnp.int32, (width, width), 0)
    part = place // block
    mirrored = jnp.zeros_like(part)
    for bit in range(bits):
        mirrored = mirrored | (((part >> bit) & 1) << (bits - 1 - bit))
    wanted = (mirrored ^ lax.axis_index("dp")) * block + place % block
    return (feature == wanted).astype(jnp.bfloat16)


LINK_BYTES_US = 90e3
CORE_BYTES_US = 500e3
HOP_US = 1.5
PARTS = 6


class Gather:
    def __init__(self, shapes, spans, flips, bits):
        self.shapes = shapes
        self.spans = spans
        self.bits = bits
        self.pieces = []
        self.steps = []
        for array, (shape, flip_first) in enumerate(zip(shapes, flips)):
            lanes = shape[2] // 128
            edges = [128 * (lanes * part // PARTS) for part in range(PARTS + 1)]
            for part in range(PARTS):
                flip = (part + flip_first) % 2 == 1
                self.pieces.append((array, edges[part], edges[part + 1] - edges[part], flip))
                self.steps.append(self.plan(flip))
        self.slots = {}
        for piece, plan in enumerate(self.steps):
            first, last = spans[self.pieces[piece][0]]
            for step in range(first, last + 1):
                for run in range(len(plan[step][1])):
                    self.slots[piece, step, run] = len(self.slots)

    def plan(self, flip):
        order = list(reversed(range(self.bits)))
        if flip:
            order[self.bits - 3], order[self.bits - 2] = 1, 2
        held = [0]
        plan = []
        for bit in order:
            offset = 1 << (self.bits - 1 - bit)
            runs = []
            for block in held:
                if runs and runs[-1][0] + runs[-1][1] == block:
                    runs[-1][1] += 1
                else:
                    runs.append([block, 1])
            plan.append((bit, [(first, count, first + offset) for first, count in runs]))
            held = sorted(held + [block + offset for block in held])
        return plan

    def timetable(self):
        free = {}
        ready = {array: (0.0, array, span[0]) for array, span in enumerate(self.spans)}
        events = []
        while ready:
            time, array, step = min(ready.values())
            done = time
            for piece, (owner, _, columns, _) in enumerate(self.pieces):
                if owner != array:
                    continue
                bit, runs = self.steps[piece][step]
                link = min(bit, 3)
                size = sum(count for _, count, _ in runs) * self.shapes[array][1] * columns * 2
                if bit == 0:
                    span = size / CORE_BYTES_US
                else:
                    span = size * (4 if bit == 4 else 2) / LINK_BYTES_US
                events.append((time, piece, step))
                free[link] = max(time, free.get(link, 0.0)) + span
                done = max(done, free[link])
            if step == self.spans[array][1]:
                del ready[array]
            else:
                ready[array] = (done + HOP_US, array, step + 1)
        return events

    def scratch(self):
        count = len(self.slots)
        return [
            pltpu.SemaphoreType.DMA((count,)),
            pltpu.SemaphoreType.DMA((count,)),
            pltpu.SemaphoreType.DMA((len(self.pieces),)),
        ]

    def in_specs(self):
        return [
            pl.BlockSpec(memory_space=pl.ANY if span[0] else pltpu.VMEM) for span in self.spans
        ]

    def out_specs(self):
        return [pl.BlockSpec(memory_space=pl.ANY)] * len(self.shapes)

    def out_shape(self):
        return [jax.ShapeDtypeStruct(shape, jnp.bfloat16) for shape in self.shapes]

    def aliases(self, inputs, outputs):
        return {
            inputs + array: outputs + array for array, span in enumerate(self.spans) if span[0]
        }

    def bind(self, shards, dests, sems):
        self.shards, self.dests = shards, dests
        self.send_sem, self.recv_sem, self.own_sem = sems

    def partner(self, bit):
        me = lax.axis_index("dp")
        return me + (1 << bit) * (1 - 2 * ((me // (1 << bit)) % 2))

    def copies(self, piece, step):
        array, start, columns, _ = self.pieces[piece]
        bit, runs = self.steps[piece][step]
        dest = self.dests[array]
        lanes = pl.ds(start, columns)
        made = []
        for run, (first, count, target) in enumerate(runs):
            slot = self.slots[piece, step, run]
            if step == 0:
                source = self.shards[array].at[:, :, lanes]
            else:
                source = dest.at[pl.ds(first, count), :, lanes]
            made.append(
                pltpu.make_async_remote_copy(
                    src_ref=source,
                    dst_ref=dest.at[pl.ds(target, count), :, lanes],
                    send_sem=self.send_sem.at[slot],
                    recv_sem=self.recv_sem.at[slot],
                    device_id=(self.partner(bit),),
                    device_id_type=pl.DeviceIdType.MESH,
                )
            )
        return made

    def own(self, piece):
        array, start, columns, _ = self.pieces[piece]
        lanes = pl.ds(start, columns)
        return pltpu.make_async_copy(
            self.shards[array].at[:, :, lanes],
            self.dests[array].at[pl.ds(0, 1), :, lanes],
            self.own_sem.at[piece],
        )

    def begin(self):
        barrier = pltpu.get_barrier_semaphore()
        for bit in range(self.bits):
            pl.semaphore_signal(
                barrier,
                inc=1,
                device_id=(self.partner(bit),),
                device_id_type=pl.DeviceIdType.MESH,
            )
        pl.semaphore_wait(barrier, self.bits)
        for piece in range(len(self.pieces)):
            if self.first(piece) == 0:
                self.own(piece).start()

    def first(self, piece):
        return self.spans[self.pieces[piece][0]][0]

    def last(self, piece):
        return self.spans[self.pieces[piece][0]][1]

    def advance(self, piece, step):
        if step == 1 and self.first(piece) == 0:
            self.own(piece).wait()
        if step > self.first(piece):
            for copy in self.copies(piece, step - 1):
                copy.wait_recv()
        for copy in self.copies(piece, step):
            copy.start()

    def finish(self):
        for piece in range(len(self.pieces)):
            for copy in self.copies(piece, self.last(piece)):
                copy.wait_recv()
        for piece in range(len(self.pieces)):
            for step in range(self.first(piece), self.last(piece) + 1):
                for copy in self.copies(piece, step):
                    copy.wait_send()


def carried(body, gather, inputs, outputs, prefetch, steps, step_us, place):
    arrays = len(gather.shapes)
    agenda = [[] for _ in range(steps)]
    for time, piece, step in gather.timetable():
        agenda[min(steps - 1, int(-(-time // step_us)))].append((piece, step))

    def kernel(*refs):
        refs = list(refs)
        cut = prefetch + inputs
        ahead, refs = refs[:cut], refs[cut:]
        shards, refs = refs[:arrays], refs[arrays:]
        results, refs = refs[:outputs], refs[outputs:]
        dests, sems = refs[:arrays], refs[arrays:]
        gather.bind(shards, dests, sems)
        here = place()
        for index, moves in enumerate(agenda):
            if index and not moves:
                continue

            @pl.when(here == index)
            def _(index=index, moves=moves):
                if index == 0:
                    gather.begin()
                for piece, step in moves:
                    gather.advance(piece, step)

        body(*ahead, *results)

        @pl.when(here == steps - 1)
        def _():
            gather.finish()

    return kernel


def gather_kernel(gather, arrays, *refs):
    gather.bind(refs[:arrays], refs[arrays : 2 * arrays], refs[2 * arrays :])
    gather.begin()
    for _, piece, step in gather.timetable():
        gather.advance(piece, step)
    gather.finish()


def gather_alone(gather, shards, collective):
    return pl.pallas_call(
        functools.partial(gather_kernel, gather, len(shards)),
        in_specs=gather.in_specs(),
        out_specs=gather.out_specs(),
        out_shape=gather.out_shape(),
        scratch_shapes=gather.scratch(),
        input_output_aliases=gather.aliases(0, 0),
        compiler_params=pltpu.CompilerParams(collective_id=collective, has_side_effects=True),
        name="gather",
    )(*shards)


def head_lanes(which):
    return lax.broadcasted_iota(jnp.int32, (1, PAIR), 1) // HEAD_DIM == which


def attend_kernel(len_ref, q_ref, k_ref, v_ref, ctx_ref):
    length = len_ref[pl.program_id(0)]
    seq = k_ref.shape[0]
    query = q_ref[...] * jnp.bfloat16(HEAD_DIM ** (-0.5))
    keys = k_ref[...]
    values = v_ref[...]
    open_keys = lax.broadcasted_iota(jnp.int32, (1, seq), 1) < length
    picked = []
    for which in range(2):
        lanes = head_lanes(which)
        scores = project_back(jnp.where(lanes, query, jnp.zeros_like(query)), keys)
        scores = jnp.where(open_keys, scores, MASK_VALUE)
        expo = jnp.exp(scores - jnp.max(scores, axis=-1, keepdims=True))
        chance = expo * (1.0 / jnp.sum(expo, axis=-1, keepdims=True))
        picked.append(project(lowered(chance), values))
    ctx_ref[...] = lowered(jnp.where(head_lanes(0), picked[0], picked[1]))


def attend(lengths, qk, values, seq, shards=(), gather=None, collective=None):
    rows, width = values.shape
    pairs = width // PAIR
    flops = 4 * rows * seq * width
    body, more_in, more_out, more_shape, scratch, params = attend_kernel, [], [], [], [], None
    aliases = {}
    if gather is not None:
        steps = rows // seq * pairs
        body = carried(
            attend_kernel,
            gather,
            3,
            1,
            1,
            steps,
            1.5,
            lambda: pl.program_id(0) * pairs + pl.program_id(1),
        )
        more_in, more_out, more_shape = gather.in_specs(), gather.out_specs(), gather.out_shape()
        scratch, aliases = gather.scratch(), gather.aliases(4, 1)
        params = pltpu.CompilerParams(collective_id=collective, has_side_effects=True)
    result = pl.pallas_call(
        body,
        grid_spec=pltpu.PrefetchScalarGridSpec(
            num_scalar_prefetch=1,
            grid=(rows // seq, pairs),
            in_specs=[
                pl.BlockSpec((seq, PAIR), lambda s, h, n: (s, h)),
                pl.BlockSpec((seq, PAIR), lambda s, h, n: (s, pairs + h)),
                pl.BlockSpec((seq, PAIR), lambda s, h, n: (s, h)),
            ]
            + more_in,
            out_specs=[pl.BlockSpec((seq, PAIR), lambda s, h, n: (s, h))] + more_out,
            scratch_shapes=scratch,
        ),
        out_shape=[jax.ShapeDtypeStruct((rows, width), jnp.bfloat16)] + more_shape,
        input_output_aliases=aliases,
        compiler_params=params,
        cost_estimate=pl.CostEstimate(
            flops=8 * flops, bytes_accessed=8 * rows * width, transcendentals=rows * seq * 12
        ),
        name="attend",
    )(lengths, qk, qk, values, *shards)
    return result[0], result[1:]


def attend_back_kernel(len_ref, q_ref, k_ref, v_ref, g_ref, dq_ref, dk_ref, dv_ref):
    length = len_ref[pl.program_id(0)]
    seq = k_ref.shape[0]
    query = q_ref[...] * jnp.bfloat16(HEAD_DIM ** (-0.5))
    keys = k_ref[...]
    values = v_ref[...]
    grads = g_ref[...]
    open_keys = lax.broadcasted_iota(jnp.int32, (seq, 1), 0) < length
    parts = []
    for which in range(2):
        lanes = head_lanes(which)
        scores = project_back(keys, jnp.where(lanes, query, jnp.zeros_like(query)))
        scores = jnp.where(open_keys, scores, MASK_VALUE)
        expo = jnp.exp(scores - jnp.max(scores, axis=0, keepdims=True))
        chance = expo * (1.0 / jnp.sum(expo, axis=0, keepdims=True))
        grad_chance = project_back(values, jnp.where(lanes, grads, jnp.zeros_like(grads)))
        weighed = jnp.sum(chance * grad_chance, axis=0, keepdims=True)
        grad_scores = lowered(chance * (grad_chance - weighed))
        parts.append(
            (
                outer_sum(grad_scores, keys) * HEAD_DIM ** (-0.5),
                project(grad_scores, query),
                project(lowered(chance), grads),
            )
        )
    first = head_lanes(0)
    for index, out_ref in enumerate((dq_ref, dk_ref, dv_ref)):
        out_ref[...] = lowered(jnp.where(first, parts[0][index], parts[1][index]))


def attend_back(lengths, qk, values, grads, seq):
    rows, width = values.shape
    pairs = width // PAIR
    flops = 10 * rows * seq * width
    spec = pl.BlockSpec((seq, PAIR), lambda s, h, n: (s, h))
    shape = jax.ShapeDtypeStruct((rows, width), jnp.bfloat16)
    return pl.pallas_call(
        attend_back_kernel,
        grid_spec=pltpu.PrefetchScalarGridSpec(
            num_scalar_prefetch=1,
            grid=(rows // seq, pairs),
            in_specs=[
                spec,
                pl.BlockSpec((seq, PAIR), lambda s, h, n: (s, pairs + h)),
                spec,
                spec,
            ],
            out_specs=[spec, spec, spec],
        ),
        out_shape=[shape, shape, shape],
        cost_estimate=pl.CostEstimate(
            flops=8 * flops, bytes_accessed=14 * rows * width, transcendentals=rows * seq * 12
        ),
        name="attend_back",
    )(lengths, qk, qk, values, grads)


def expand_kernel(h_ref, w_ref, b_ref, u_ref, slope_ref):
    inner = project(h_ref[...], w_ref[...]) + b_ref[...]
    bell = jnp.exp(inner * inner * -0.5)
    step = 1.0 / (1.0 + TAIL_P * jnp.abs(inner))
    poly = jnp.full_like(step, TAIL_C[-1])
    for coefficient in reversed(TAIL_C[:-1]):
        poly = poly * step + coefficient
    tail = poly * step * bell
    below = jnp.where(inner >= 0, 1.0 - tail, tail)
    u_ref[...] = lowered(inner * below)
    slope_ref[...] = lowered(below + inner * bell * INV_SQRT_2PI)


def expand(normed, weight, bias, shards=(), gather=None, collective=None, tile=256):
    rows, width = normed.shape
    hidden = weight.shape[1]
    body, more_in, more_out, more_shape, scratch, params = expand_kernel, [], [], [], [], None
    aliases = {}
    if gather is not None:
        body = carried(
            expand_kernel, gather, 3, 2, 0, hidden // tile, 1.6, lambda: pl.program_id(0)
        )
        more_in, more_out, more_shape = gather.in_specs(), gather.out_specs(), gather.out_shape()
        scratch, aliases = gather.scratch(), gather.aliases(3, 2)
        params = pltpu.CompilerParams(collective_id=collective, has_side_effects=True)
    shape = jax.ShapeDtypeStruct((rows, hidden), jnp.bfloat16)
    out_spec = pl.BlockSpec((rows, tile), lambda j: (0, j))
    result = pl.pallas_call(
        body,
        grid=(hidden // tile,),
        in_specs=[
            pl.BlockSpec((rows, width), lambda j: (0, 0)),
            pl.BlockSpec((width, tile), lambda j: (0, j)),
            pl.BlockSpec((1, tile), lambda j: (0, j)),
        ]
        + more_in,
        out_specs=[out_spec, out_spec] + more_out,
        out_shape=[shape, shape] + more_shape,
        scratch_shapes=scratch,
        input_output_aliases=aliases,
        compiler_params=params,
        cost_estimate=pl.CostEstimate(
            flops=6 * rows * width * hidden,
            bytes_accessed=2 * width * hidden + 4 * rows * hidden,
            transcendentals=2 * rows * hidden,
        ),
        name="expand",
    )(normed, weight, bias, *shards)
    return result[0], result[1], result[2:]


def norm_parts(value):
    centred = value - jnp.mean(value, axis=-1, keepdims=True)
    inverse = lax.rsqrt(jnp.mean(centred * centred, axis=-1, keepdims=True) + NORM_EPS)
    return centred * inverse, inverse


def norm_back(grad, value, gain):
    unit, inverse = norm_parts(value)
    grad_gain = jnp.sum(grad * unit, axis=0)
    grad_shift = jnp.sum(grad, axis=0)
    grad_unit = grad * gain
    grad_value = inverse * (
        grad_unit
        - jnp.mean(grad_unit, axis=-1, keepdims=True)
        - unit * jnp.mean(grad_unit * unit, axis=-1, keepdims=True)
    )
    return grad_value, grad_gain, grad_shift


class Weights:
    def __init__(self, w_qk, w_vo, spread):
        width = spread.shape[0]
        self.w_qk, self.w_vo = w_qk, w_vo
        place = w_vo[:, 2 * width :]
        self.vec_plain = jnp.transpose(project(spread, place))
        self.vec_place = jnp.transpose(place.astype(jnp.float32))
        self.w_up = self.w_down = None


def layer_ahead(rows, weights, lengths, seq, during_attend, during_expand):
    width = rows.shape[1]
    plain, vec_place = weights.vec_plain, weights.vec_place
    bias_q, bias_v, bias_up = plain[0], plain[1], plain[8:12].reshape(1, -1)
    bias_qk = jnp.concatenate([bias_q, jnp.zeros_like(bias_q)])
    qk = lowered(project(rows, weights.w_qk) + bias_qk)
    values = lowered(project(rows, weights.w_vo[:, :width]) + bias_v)
    context = during_attend(lengths, qk, values, seq)
    first_sum = (
        rows.astype(jnp.float32)
        + project_back(context, weights.w_vo[:, width : 2 * width])
        + vec_place[2]
    )
    normed = lowered(norm_parts(first_sum)[0] * vec_place[3] + vec_place[4])
    active, slope = during_expand(normed, bias_up)
    second_sum = normed.astype(jnp.float32) + project_back(active, weights.w_down) + vec_place[7]
    output = lowered(norm_parts(second_sum)[0] * vec_place[5] + vec_place[6])
    return output, (qk, values, context, first_sum, normed, active, slope, second_sum)


def layer_behind(grad_out, rows, kept, weights, lengths, seq, spread):
    w_qk, w_vo, w_up, w_down = weights.w_qk, weights.w_vo, weights.w_up, weights.w_down
    vec_place = weights.vec_place
    width = rows.shape[1]
    qk, values, context, first_sum, normed, active, slope, second_sum = kept
    grad_second, gain_two, shift_two = norm_back(grad_out, second_sum, vec_place[5])
    grad_ffn = lowered(grad_second)
    bias_out = jnp.sum(grad_ffn.astype(jnp.float32), axis=0)
    down_grad = outer_scatter(grad_ffn, active, True)
    grad_inner = lowered(project(grad_ffn, w_down) * slope.astype(jnp.float32))
    bias_inner = jnp.sum(grad_inner.astype(jnp.float32), axis=0)
    up_grad = outer_scatter(normed, grad_inner, False)
    grad_normed = grad_second + project_back(grad_inner, w_up)
    grad_first, gain_one, shift_one = norm_back(grad_normed, first_sum, vec_place[3])
    grad_attn = lowered(grad_first)
    bias_attn = jnp.sum(grad_attn.astype(jnp.float32), axis=0)
    out_grad = outer_scatter(grad_attn, context, True)
    grad_context = lowered(project(grad_attn, w_vo[:, width : 2 * width]))
    grad_query, grad_keys, grad_values = attend_back(lengths, qk, values, grad_context, seq)
    bias_query = jnp.sum(grad_query.astype(jnp.float32), axis=0)
    bias_value = jnp.sum(grad_values.astype(jnp.float32), axis=0)
    value_grad = outer_scatter(rows, grad_values, True)
    query_grad = outer_scatter(rows, grad_query, False)
    key_grad = outer_scatter(rows, grad_keys, False)
    grad_rows = grad_first + project_back(grad_query, w_qk[:, :width])
    grad_rows = grad_rows + project_back(grad_keys, w_qk[:, width:])
    grad_rows = grad_rows + project_back(grad_values, w_vo[:, :width])
    plain = jnp.concatenate(
        [jnp.stack([bias_query, bias_value]), bias_inner.reshape(-1, width)], axis=0
    )
    placed = jnp.dot(plain, spread.astype(jnp.float32), precision=lax.Precision.HIGHEST)
    vec_grad = jnp.stack(
        [
            placed[0],
            placed[1],
            bias_attn,
            gain_one,
            shift_one,
            gain_two,
            shift_two,
            bias_out,
            placed[2],
            placed[3],
            placed[4],
            placed[5],
        ],
        axis=1,
    )
    attn_grad = jnp.concatenate([query_grad, key_grad, value_grad, out_grad], axis=1)
    ffn_grad = jnp.concatenate([up_grad, down_grad], axis=1)
    return grad_rows, (attn_grad, ffn_grad, vec_grad)


def ahead_permuted(rows, shards_all, spread, lengths, seq):
    layer_inputs, kept_all, weights_all = [], [], []
    for shards in shards_all:
        weights = Weights(gather_rows(shards[0], False), gather_rows(shards[1], True), spread)
        weights.w_up = gather_rows(shards[2], False)
        weights.w_down = gather_rows(shards[3], True)
        layer_inputs.append(rows)
        rows, kept = layer_ahead(
            rows,
            weights,
            lengths,
            seq,
            lambda *operands: attend(*operands)[0],
            lambda normed, bias, weights=weights: expand(normed, weights.w_up, bias)[:2],
        )
        kept_all.append(kept)
        weights_all.append(weights)
    return rows, layer_inputs, kept_all, weights_all


def ahead_carried(rows, shards_all, spread, lengths, seq):
    devices = lax.axis_size("dp")
    bits = bit_count(devices)
    layers = len(shards_all)

    along = 2
    last = bits - 1
    arrays = {}

    def plan(*wanted):
        wanted = [item for item in wanted if item[0] < layers]
        operands, shapes = [], []
        for layer, index, first, _ in wanted:
            shard = shards_all[layer][index][None]
            operands.append(arrays[layer, index] if first else shard)
            shapes.append((devices,) + shard.shape[1:])
        spans = [item[2:] for item in wanted]
        flips = [item[1] % 2 for item in wanted]

        def keep(results):
            for (layer, index, _, _), result in zip(wanted, results):
                arrays[layer, index] = result

        return operands, Gather(shapes, spans, flips, bits), keep

    def flat(layer, index):
        array = arrays[layer, index]
        return array.reshape(-1, array.shape[2])

    operands, gather, keep = plan((0, 0, 0, last), (0, 1, 0, last), (0, 2, 0, along - 1), (1, 0, 0, along - 1))
    keep(gather_alone(gather, operands, 0))
    layer_inputs, kept_all, weights_all = [], [], []
    for layer in range(layers):
        weights = Weights(flat(layer, 0), flat(layer, 1), spread)

        def during_attend(lengths, qk, values, seq):
            operands, gather, keep = plan(
                (layer, 2, along, last),
                (layer + 1, 0, along, last),
                (layer, 3, 0, along - 1),
                (layer + 1, 1, 0, along - 1),
            )
            context, arrived = attend(
                lengths, qk, values, seq, operands, gather, 1 + 2 * layer
            )
            keep(arrived)
            weights.w_up = flat(layer, 2)
            return context

        def during_expand(normed, bias):
            operands, gather, keep = plan(
                (layer, 3, along, last),
                (layer + 1, 1, along, last),
                (layer + 1, 2, 0, along - 1),
                (layer + 2, 0, 0, along - 1),
            )
            active, slope, arrived = expand(
                normed, weights.w_up, bias, operands, gather, 2 + 2 * layer
            )
            keep(arrived)
            weights.w_down = flat(layer, 3)
            return active, slope

        layer_inputs.append(rows)
        rows, kept = layer_ahead(rows, weights, lengths, seq, during_attend, during_expand)
        kept_all.append(kept)
        weights_all.append(weights)
    return rows, layer_inputs, kept_all, weights_all


def adam_step(param, first, second, grad):
    first_new = 0.9 * first + 0.1 * grad
    second_new = 0.98 * second + 0.02 * grad * grad
    first_hat = first_new / (1.0 - 0.9**10)
    second_hat = second_new / (1.0 - 0.98**10)
    direction = first_hat / (jnp.sqrt(second_hat) + 1e-08) + 0.01 * param
    return (direction, first_new, second_new)


def local(
    tokens,
    cotangent,
    lengths,
    counts,
    attn_w,
    ffn_w,
    vec_w,
    attn_m,
    ffn_m,
    vec_m,
    attn_v,
    ffn_v,
    vec_v,
):
    row_total, width = tokens.shape
    seq = row_total // lengths.shape[0]
    layers = attn_w.shape[0]
    hidden = ffn_w.shape[2] // 2
    vec_rows = vec_w.shape[1]
    micro = lax.broadcasted_iota(jnp.int32, (row_total, 1), 0) // (seq * SEQ_MB)
    live = micro < counts[0]
    spread = order_matrix(width)
    shards_all = []
    for layer in range(layers):
        attn = lowered(attn_w[layer])
        ffn = lowered(ffn_w[layer])
        vec = jnp.pad(jnp.transpose(lowered(vec_w[layer])), ((0, 0), (0, 128 - vec_rows)))
        shards_all.append(
            (
                attn[:, : 2 * width],
                jnp.concatenate([attn[:, 2 * width :], vec], axis=1),
                ffn[:, :hidden],
                ffn[:, hidden:],
            )
        )
    ahead = ahead_carried if attn_w.shape[1] % 8 == 0 else ahead_permuted
    rows = lowered(project(tokens, spread))
    rows, layer_inputs, kept_all, weights_all = ahead(rows, shards_all, spread, lengths, seq)
    activations = lowered(jnp.where(live, project_back(rows, spread), 0.0))
    grad_rows = jnp.where(live, project(cotangent, spread), 0.0)
    summed_all = [None] * layers
    for layer in reversed(range(layers)):
        grad_rows, summed_all[layer] = layer_behind(
            grad_rows,
            layer_inputs[layer],
            kept_all[layer],
            weights_all[layer],
            lengths,
            seq,
            spread,
        )
    high = lax.reduce_precision(grad_rows, 8, 7)
    in_grad = project_back(lowered(high), spread) + project_back(lowered(grad_rows - high), spread)
    vec_local = jnp.concatenate([summed_all[index][2] for index in range(layers)], axis=1)
    half = width // 2
    vec_sum = scatter_rows(vec_local[:half], vec_local[half:], False, jnp.float32)
    vec_sum = jnp.transpose(vec_sum).reshape(layers, vec_rows, -1)
    factor = float(row_total * lax.axis_size("dp")) ** (-0.5)
    attn_grad = jnp.stack([summed_all[index][0] for index in range(layers)]) * factor
    ffn_grad = jnp.stack([summed_all[index][1] for index in range(layers)]) * factor
    vec_grad = vec_sum * factor
    attn_step, attn_m_new, attn_v_new = adam_step(attn_w, attn_m, attn_v, attn_grad)
    ffn_step, ffn_m_new, ffn_v_new = adam_step(ffn_w, ffn_m, ffn_v, ffn_grad)
    vec_step, vec_m_new, vec_v_new = adam_step(vec_w, vec_m, vec_v, vec_grad)
    return (
        activations,
        in_grad,
        attn_grad,
        ffn_grad,
        vec_grad,
        attn_step,
        ffn_step,
        vec_step,
        attn_m_new,
        ffn_m_new,
        vec_m_new,
        attn_v_new,
        ffn_v_new,
        vec_v_new,
    )


def solution(mesh):
    rows = P("dp", None)
    weight = P(None, "dp", None)
    vector = P(None, None, "dp")
    in_specs = (rows, rows, P("dp"), P("dp")) + (weight, weight, vector) * 3
    out_specs = (rows, rows) + (weight, weight, vector) * 4
    return jax.shard_map(local, mesh=mesh, in_specs=in_specs, out_specs=out_specs, check_vma=False)
```

```python
import functools

import jax
import jax.numpy as jnp
from jax import lax
from jax.experimental import pallas as pl
from jax.experimental.pallas import tpu as pltpu
from jax.sharding import PartitionSpec as P

HEAD_DIM = 64
SEQ_MB = 1
PAIR = 2 * HEAD_DIM

NORM_EPS = 1e-05
MASK_VALUE = -1e30

TAIL_P = 0.275
TAIL_C = (0.1178092576, 0.04211145346, 0.3339323636, -0.3309935012, 0.4519987806, -0.1148583494)
INV_SQRT_2PI = 0.3989422804014327


def lowered(value):
    return value.astype(jnp.bfloat16)


def project(left, right):
    return jnp.dot(left, right, preferred_element_type=jnp.float32)


def project_back(left, right):
    return lax.dot_general(
        left, right, (((1,), (1,)), ((), ())), preferred_element_type=jnp.float32
    )


def outer_sum(left, right):
    return lax.dot_general(
        left, right, (((0,), (0,)), ((), ())), preferred_element_type=jnp.float32
    )


def bit_count(devices):
    bits = devices.bit_length() - 1
    assert 1 << bits == devices
    return bits


def swap(value, bit):
    devices = lax.axis_size("dp")
    return lax.ppermute(value, "dp", [(i, i ^ (1 << bit)) for i in range(devices)])


def gather_rows(shard, flip):
    bits = bit_count(lax.axis_size("dp"))
    rows = shard
    for bit in reversed(range(3 if flip else 0, bits)):
        rows = jnp.concatenate([rows, swap(rows, bit)], axis=0)
    if flip:
        height, width = rows.shape
        rows = jnp.concatenate([rows[None], swap(rows, 1)[None]], axis=0)
        rows = jnp.concatenate([rows[:, None], swap(rows, 2)[:, None]], axis=1)
        rows = rows.reshape(4 * height, width)
        rows = jnp.concatenate([rows, swap(rows, 0)], axis=0)
    return rows


def scatter_rows(keep, send, flip, wire):
    bits = bit_count(lax.axis_size("dp"))
    total = keep + swap(send.astype(wire), 0).astype(jnp.float32)
    start = 1
    if flip:
        total = total.astype(wire)
        height, width = total.shape
        quarter = total.reshape(2, 2, height // 4, width)
        total = quarter[:, 0].astype(jnp.float32) + swap(quarter[:, 1], 2).astype(jnp.float32)
        total = total.astype(wire)
        total = total[0].astype(jnp.float32) + swap(total[1], 1).astype(jnp.float32)
        start = 3
    for bit in range(start, bits):
        total = total.astype(wire)
        half = total.shape[0] // 2
        total = total[:half].astype(jnp.float32) + swap(total[half:], bit).astype(jnp.float32)
    return total


def outer_scatter(left, right, flip):
    half = left.shape[1] // 2
    send = lowered(outer_sum(left[:, half:], right))
    keep = outer_sum(left[:, :half], right)
    return scatter_rows(keep, send, flip, jnp.bfloat16)


def order_matrix(width):
    devices = lax.axis_size("dp")
    bits = bit_count(devices)
    block = width // devices
    place = lax.broadcasted_iota(jnp.int32, (width, width), 1)
    feature = lax.broadcasted_iota(jnp.int32, (width, width), 0)
    part = place // block
    mirrored = jnp.zeros_like(part)
    for bit in range(bits):
        mirrored = mirrored | (((part >> bit) & 1) << (bits - 1 - bit))
    wanted = (mirrored ^ lax.axis_index("dp")) * block + place % block
    return (feature == wanted).astype(jnp.bfloat16)


LINK_BYTES_US = 90e3
CORE_BYTES_US = 500e3
HOP_US = 1.5
PARTS = 6
VMEM_BYTES = 60 << 20


class Gather:
    def __init__(self, shapes, spans, flips, bits):
        self.shapes = shapes
        self.arrays = len(shapes)
        self.spans = spans
        self.bits = bits
        self.pieces = []
        self.steps = []
        for array, (shape, flip_first) in enumerate(zip(shapes, flips)):
            lanes = shape[2] // 128
            edges = [128 * (lanes * part // PARTS) for part in range(PARTS + 1)]
            for part in range(PARTS):
                flip = (part + flip_first) % 2 == 1
                self.pieces.append((array, edges[part], edges[part + 1] - edges[part], flip))
                self.steps.append(self.plan(flip))
        self.slots = {}
        for piece, plan in enumerate(self.steps):
            first, last = spans[self.pieces[piece][0]]
            for step in range(first, last + 1):
                for run in range(len(plan[step][1])):
                    self.slots[piece, step, run] = len(self.slots)

    def plan(self, flip):
        order = list(reversed(range(self.bits)))
        if flip:
            order[self.bits - 3], order[self.bits - 2] = 1, 2
        held = [0]
        plan = []
        for bit in order:
            offset = 1 << (self.bits - 1 - bit)
            runs = []
            for block in held:
                if runs and runs[-1][0] + runs[-1][1] == block:
                    runs[-1][1] += 1
                else:
                    runs.append([block, 1])
            plan.append((bit, [(first, count, first + offset) for first, count in runs]))
            held = sorted(held + [block + offset for block in held])
        return plan

    def timetable(self):
        free = {}
        ready = {array: (0.0, array, span[0]) for array, span in enumerate(self.spans)}
        events = []
        while ready:
            time, array, step = min(ready.values())
            done = time
            for piece, (owner, _, columns, _) in enumerate(self.pieces):
                if owner != array:
                    continue
                bit, runs = self.steps[piece][step]
                link = min(bit, 3)
                size = sum(count for _, count, _ in runs) * self.shapes[array][1] * columns * 2
                if bit == 0:
                    span = size / CORE_BYTES_US
                else:
                    span = size * (4 if bit == 4 else 2) / LINK_BYTES_US
                events.append((time, piece, step))
                free[link] = max(time, free.get(link, 0.0)) + span
                done = max(done, free[link])
            if step == self.spans[array][1]:
                del ready[array]
            else:
                ready[array] = (done + HOP_US, array, step + 1)
        return events

    def scratch(self):
        count = len(self.slots)
        return [
            pltpu.SemaphoreType.DMA((count,)),
            pltpu.SemaphoreType.DMA((count,)),
            pltpu.SemaphoreType.DMA((len(self.pieces),)),
        ]

    def in_specs(self):
        return [
            pl.BlockSpec(memory_space=pl.ANY if span[0] else pltpu.VMEM) for span in self.spans
        ]

    def out_specs(self):
        return [pl.BlockSpec(memory_space=pl.ANY)] * len(self.shapes)

    def out_shape(self):
        return [jax.ShapeDtypeStruct(shape, jnp.bfloat16) for shape in self.shapes]

    def aliases(self, inputs, outputs):
        return {
            inputs + array: outputs + array for array, span in enumerate(self.spans) if span[0]
        }

    def bind(self, shards, dests, sems):
        self.shards, self.dests = shards, dests
        self.send_sem, self.recv_sem, self.own_sem = sems

    def partner(self, bit):
        me = lax.axis_index("dp")
        return me + (1 << bit) * (1 - 2 * ((me // (1 << bit)) % 2))

    def copies(self, piece, step):
        array, start, columns, _ = self.pieces[piece]
        bit, runs = self.steps[piece][step]
        dest = self.dests[array]
        lanes = pl.ds(start, columns)
        made = []
        for run, (first, count, target) in enumerate(runs):
            slot = self.slots[piece, step, run]
            if step == 0:
                source = self.shards[array].at[:, :, lanes]
            else:
                source = dest.at[pl.ds(first, count), :, lanes]
            made.append(
                pltpu.make_async_remote_copy(
                    src_ref=source,
                    dst_ref=dest.at[pl.ds(target, count), :, lanes],
                    send_sem=self.send_sem.at[slot],
                    recv_sem=self.recv_sem.at[slot],
                    device_id=(self.partner(bit),),
                    device_id_type=pl.DeviceIdType.MESH,
                )
            )
        return made

    def own(self, piece):
        array, start, columns, _ = self.pieces[piece]
        lanes = pl.ds(start, columns)
        return pltpu.make_async_copy(
            self.shards[array].at[:, :, lanes],
            self.dests[array].at[pl.ds(0, 1), :, lanes],
            self.own_sem.at[piece],
        )

    def begin(self):
        barrier = pltpu.get_barrier_semaphore()
        for bit in range(self.bits):
            pl.semaphore_signal(
                barrier,
                inc=1,
                device_id=(self.partner(bit),),
                device_id_type=pl.DeviceIdType.MESH,
            )
        pl.semaphore_wait(barrier, self.bits)
        for piece in range(len(self.pieces)):
            if self.first(piece) == 0:
                self.own(piece).start()

    def first(self, piece):
        return self.spans[self.pieces[piece][0]][0]

    def last(self, piece):
        return self.spans[self.pieces[piece][0]][1]

    def advance(self, piece, step):
        if step == 1 and self.first(piece) == 0:
            self.own(piece).wait()
        if step > self.first(piece):
            for copy in self.copies(piece, step - 1):
                copy.wait_recv()
        for copy in self.copies(piece, step):
            copy.start()

    def finish(self):
        for piece in range(len(self.pieces)):
            for copy in self.copies(piece, self.last(piece)):
                copy.wait_recv()
        for piece in range(len(self.pieces)):
            for step in range(self.first(piece), self.last(piece) + 1):
                for copy in self.copies(piece, step):
                    copy.wait_send()


class Scatter:
    def __init__(self, arrays):
        self.given = arrays
        self.arrays = len(arrays)
        self.pieces = []
        for array, (columns, _, _, parts, first) in enumerate(arrays):
            lanes = columns // 128
            edges = [128 * (lanes * part // parts) for part in range(parts + 1)]
            for part in range(parts):
                flip = (part + first) % 2
                self.pieces.append((array, edges[part], edges[part + 1] - edges[part], flip))

    def set_rows(self, rows):
        self.rows = rows
        return self

    def range_of(self, array):
        return {"full": (0, 4), "front": (0, 2), "back": (3, 4)}[self.given[array][2]]

    def link(self, step, flip):
        return (0, 2, 1, 3, 4)[step] if flip else (0, 1, 2, 3, 4)[step]

    def timetable(self):
        free = {}
        ready = {array: (0.0, array, self.range_of(array)[0]) for array in range(self.arrays)}
        events = []
        while ready:
            time, array, step = min(ready.values())
            done = time
            last = self.range_of(array)[1]
            for piece, (owner, _, columns, flip) in enumerate(self.pieces):
                if owner != array:
                    continue
                events.append((time, piece, step))
                if step > last:
                    continue
                bit = self.link(step, flip)
                size = (self.rows >> (step + 1)) * columns * jnp.dtype(self.given[array][1]).itemsize
                if bit == 0:
                    span = size / CORE_BYTES_US
                else:
                    span = size * (4 if bit == 4 else 2) / LINK_BYTES_US
                link = min(bit, 3)
                free[link] = max(time, free.get(link, 0.0)) + span
                done = max(done, free[link])
            if step > last:
                del ready[array]
            else:
                ready[array] = (done + HOP_US, array, step + 1)
        return events

    def in_specs(self):
        return [
            pl.BlockSpec(memory_space=pltpu.VMEM if given[2] == "back" else pl.ANY)
            for given in self.given
        ]

    def out_specs(self):
        return [pl.BlockSpec(memory_space=pltpu.VMEM)] * self.arrays

    def out_shape(self):
        return [
            jax.ShapeDtypeStruct((self.rows // 8, columns), kind)
            if span == "front"
            else jax.ShapeDtypeStruct((self.rows // 32, columns), jnp.float32)
            for columns, kind, span, _, _ in self.given
        ]

    def aliases(self, inputs, outputs):
        return {}

    def scratch(self):
        made = []
        for columns, kind, span, _, _ in self.given:
            if span != "back":
                made += [pltpu.VMEM((self.rows // 2, columns), kind)] * 2
                made.append(pltpu.VMEM((self.rows // 4, columns), kind))
                made.append(pltpu.VMEM((self.rows // 8, columns), kind))
            if span != "front":
                made.append(pltpu.VMEM((self.rows // 16, columns), kind))
                made += [pltpu.VMEM((self.rows // 32, columns), kind)] * 2
                made.append(pltpu.VMEM((self.rows // 32, columns), jnp.float32))
        count = len(self.pieces)
        made += [pltpu.SemaphoreType.DMA((count * 6,))] * 2
        made.append(pltpu.SemaphoreType.DMA((count,)))
        return made

    def bind(self, sources, results, scratch):
        self.sources, self.results = sources, results
        scratch = list(scratch)
        self.part, self.landing, self.leaving, self.own = {}, {}, {}, {}
        for array, given in enumerate(self.given):
            if given[2] != "back":
                self.part[array], self.landing[array, 0] = scratch.pop(0), scratch.pop(0)
                self.landing[array, 1], self.landing[array, 2] = scratch.pop(0), scratch.pop(0)
            else:
                self.part[array] = sources[array]
            if given[2] != "front":
                self.landing[array, 3] = scratch.pop(0)
                self.landing[array, 4], self.leaving[array] = scratch.pop(0), scratch.pop(0)
                self.own[array] = scratch.pop(0)
        self.send_sem, self.recv_sem, self.own_sem = scratch

    def partner(self, bit):
        me = lax.axis_index("dp")
        return me + (1 << bit) * (1 - 2 * ((me // (1 << bit)) % 2))

    def begin(self):
        barrier = pltpu.get_barrier_semaphore()
        for bit in range(5):
            pl.semaphore_signal(
                barrier,
                inc=1,
                device_id=(self.partner(bit),),
                device_id_type=pl.DeviceIdType.MESH,
            )
        pl.semaphore_wait(barrier, 5)

    def fetch(self, piece):
        array, start, columns, _ = self.pieces[piece]
        lanes = pl.ds(start, columns)
        half = self.rows // 2
        return pltpu.make_async_copy(
            self.sources[array].at[pl.ds(0, half), lanes],
            self.part[array].at[:, lanes],
            self.own_sem.at[piece],
        )

    def copies(self, piece, step):
        array, start, columns, flip = self.pieces[piece]
        lanes = pl.ds(start, columns)
        size = self.rows >> (step + 1)
        source = self.part[array]
        if step == 0:
            source, runs = self.sources[array], [(size, 0, size)]
        elif step == 1 and flip:
            runs = [(size // 2, 0, size // 2), (3 * size // 2, size // 2, size // 2)]
        elif step == 4:
            source, runs = self.leaving[array], [(0, 0, size)]
        elif step == 2 and flip:
            runs = [(2 * size, 0, size)]
        else:
            runs = [(size, 0, size)]
        made = []
        for run, (first, target, count) in enumerate(runs):
            slot = piece * 6 + (step if run == 0 else 5)
            made.append(
                pltpu.make_async_remote_copy(
                    src_ref=source.at[pl.ds(first, count), lanes],
                    dst_ref=self.landing[array, step].at[pl.ds(target, count), lanes],
                    send_sem=self.send_sem.at[slot],
                    recv_sem=self.recv_sem.at[slot],
                    device_id=(self.partner(self.link(step, flip)),),
                    device_id_type=pl.DeviceIdType.MESH,
                )
            )
        return made

    def add(self, piece, step):
        array, start, columns, flip = self.pieces[piece]
        lanes = pl.ds(start, columns)
        part, landed = self.part[array], self.landing[array, step]
        size = self.rows >> (step + 1)
        if step == 4:
            self.results[array][:, lanes] = self.own[array][:, lanes] + landed[:, lanes].astype(
                jnp.float32
            )
        elif step == 3:
            total = part[pl.ds(0, size), lanes].astype(jnp.float32) + landed[:, lanes].astype(
                jnp.float32
            )
            self.own[array][:, lanes] = total[: size // 2]
            self.leaving[array][:, lanes] = total[size // 2 :].astype(self.given[array][1])
        elif step == 2 and self.given[array][2] == "front":
            self.results[array][:, lanes] = part[pl.ds(0, size), lanes] + landed[:, lanes]
        else:
            block = self.rows // 16
            skip = size // 2 if step == 1 and flip else None

            def body(index, carry):
                from_row = pl.multiple_of(index * block, block)
                row = from_row
                if skip:
                    row = pl.multiple_of(from_row + (index // (skip // block)) * skip, block)
                part[pl.ds(row, block), lanes] = (
                    part[pl.ds(row, block), lanes] + landed[pl.ds(from_row, block), lanes]
                )
                return carry

            lax.fori_loop(0, size // block, body, 0)

    def advance(self, piece, step):
        first, last = self.range_of(self.pieces[piece][0])
        if step == 0:
            self.fetch(piece).start()
        if step > first:
            if step == 1:
                self.fetch(piece).wait()
            for copy in self.copies(piece, step - 1):
                copy.wait_recv()
            self.add(piece, step - 1)
        if step <= last:
            for copy in self.copies(piece, step):
                copy.start()

    def finish(self):
        for piece in range(len(self.pieces)):
            first, last = self.range_of(self.pieces[piece][0])
            for step in range(first, last + 1):
                for copy in self.copies(piece, step):
                    copy.wait_send()


def scatter_kernel(scatter, *refs):
    arrays = scatter.arrays
    scatter.bind(refs[:arrays], refs[arrays : 2 * arrays], refs[2 * arrays :])
    scatter.begin()
    for _, piece, step in scatter.timetable():
        scatter.advance(piece, step)
    scatter.finish()


def scatter_alone(scatter, sources, collective):
    return pl.pallas_call(
        functools.partial(scatter_kernel, scatter),
        in_specs=scatter.in_specs(),
        out_specs=scatter.out_specs(),
        out_shape=scatter.out_shape(),
        scratch_shapes=scatter.scratch(),
        compiler_params=pltpu.CompilerParams(
            collective_id=collective, has_side_effects=True, vmem_limit_bytes=VMEM_BYTES
        ),
        name="scatter",
    )(*sources)


def carried(body, gather, inputs, outputs, prefetch, steps, step_us, place):
    arrays = gather.arrays
    agenda = [[] for _ in range(steps)]
    for time, piece, step in gather.timetable():
        agenda[min(steps - 1, int(-(-time // step_us)))].append((piece, step))

    def kernel(*refs):
        refs = list(refs)
        cut = prefetch + inputs
        ahead, refs = refs[:cut], refs[cut:]
        shards, refs = refs[:arrays], refs[arrays:]
        results, refs = refs[:outputs], refs[outputs:]
        dests, sems = refs[:arrays], refs[arrays:]
        gather.bind(shards, dests, sems)
        here = place()
        for index, moves in enumerate(agenda):
            if index and not moves:
                continue

            @pl.when(here == index)
            def _(index=index, moves=moves):
                if index == 0:
                    gather.begin()
                for piece, step in moves:
                    gather.advance(piece, step)

        body(*ahead, *results)

        @pl.when(here == steps - 1)
        def _():
            gather.finish()

    return kernel


def gather_kernel(gather, arrays, *refs):
    gather.bind(refs[:arrays], refs[arrays : 2 * arrays], refs[2 * arrays :])
    gather.begin()
    for _, piece, step in gather.timetable():
        gather.advance(piece, step)
    gather.finish()


def gather_alone(gather, shards, collective):
    return pl.pallas_call(
        functools.partial(gather_kernel, gather, len(shards)),
        in_specs=gather.in_specs(),
        out_specs=gather.out_specs(),
        out_shape=gather.out_shape(),
        scratch_shapes=gather.scratch(),
        input_output_aliases=gather.aliases(0, 0),
        compiler_params=pltpu.CompilerParams(collective_id=collective, has_side_effects=True),
        name="gather",
    )(*shards)


def head_lanes(which):
    return lax.broadcasted_iota(jnp.int32, (1, PAIR), 1) // HEAD_DIM == which


def attend_kernel(len_ref, q_ref, k_ref, v_ref, ctx_ref):
    length = len_ref[pl.program_id(0)]
    seq = k_ref.shape[0]
    query = q_ref[...] * jnp.bfloat16(HEAD_DIM ** (-0.5))
    keys = k_ref[...]
    values = v_ref[...]
    open_keys = lax.broadcasted_iota(jnp.int32, (1, seq), 1) < length
    picked = []
    for which in range(2):
        lanes = head_lanes(which)
        scores = project_back(jnp.where(lanes, query, jnp.zeros_like(query)), keys)
        scores = jnp.where(open_keys, scores, MASK_VALUE)
        expo = jnp.exp(scores - jnp.max(scores, axis=-1, keepdims=True))
        chance = expo * (1.0 / jnp.sum(expo, axis=-1, keepdims=True))
        picked.append(project(lowered(chance), values))
    ctx_ref[...] = lowered(jnp.where(head_lanes(0), picked[0], picked[1]))


def attend(lengths, qk, values, seq, shards=(), gather=None, collective=None):
    rows, width = values.shape
    pairs = width // PAIR
    flops = 4 * rows * seq * width
    body, more_in, more_out, more_shape, scratch, params = attend_kernel, [], [], [], [], None
    aliases = {}
    if gather is not None:
        steps = rows // seq * pairs
        body = carried(
            attend_kernel,
            gather,
            3,
            1,
            1,
            steps,
            1.5,
            lambda: pl.program_id(0) * pairs + pl.program_id(1),
        )
        more_in, more_out, more_shape = gather.in_specs(), gather.out_specs(), gather.out_shape()
        scratch, aliases = gather.scratch(), gather.aliases(4, 1)
        params = pltpu.CompilerParams(collective_id=collective, has_side_effects=True)
    result = pl.pallas_call(
        body,
        grid_spec=pltpu.PrefetchScalarGridSpec(
            num_scalar_prefetch=1,
            grid=(rows // seq, pairs),
            in_specs=[
                pl.BlockSpec((seq, PAIR), lambda s, h, n: (s, h)),
                pl.BlockSpec((seq, PAIR), lambda s, h, n: (s, pairs + h)),
                pl.BlockSpec((seq, PAIR), lambda s, h, n: (s, h)),
            ]
            + more_in,
            out_specs=[pl.BlockSpec((seq, PAIR), lambda s, h, n: (s, h))] + more_out,
            scratch_shapes=scratch,
        ),
        out_shape=[jax.ShapeDtypeStruct((rows, width), jnp.bfloat16)] + more_shape,
        input_output_aliases=aliases,
        compiler_params=params,
        cost_estimate=pl.CostEstimate(
            flops=8 * flops, bytes_accessed=8 * rows * width, transcendentals=rows * seq * 12
        ),
        name="attend",
    )(lengths, qk, qk, values, *shards)
    return result[0], result[1:]


def attend_back_kernel(len_ref, q_ref, k_ref, v_ref, g_ref, dq_ref, dk_ref, dv_ref):
    length = len_ref[pl.program_id(0)]
    seq = k_ref.shape[0]
    query = q_ref[...] * jnp.bfloat16(HEAD_DIM ** (-0.5))
    keys = k_ref[...]
    values = v_ref[...]
    grads = g_ref[...]
    open_keys = lax.broadcasted_iota(jnp.int32, (seq, 1), 0) < length
    parts = []
    for which in range(2):
        lanes = head_lanes(which)
        scores = project_back(keys, jnp.where(lanes, query, jnp.zeros_like(query)))
        scores = jnp.where(open_keys, scores, MASK_VALUE)
        expo = jnp.exp(scores - jnp.max(scores, axis=0, keepdims=True))
        chance = expo * (1.0 / jnp.sum(expo, axis=0, keepdims=True))
        grad_chance = project_back(values, jnp.where(lanes, grads, jnp.zeros_like(grads)))
        weighed = jnp.sum(chance * grad_chance, axis=0, keepdims=True)
        grad_scores = lowered(chance * (grad_chance - weighed))
        parts.append(
            (
                outer_sum(grad_scores, keys) * HEAD_DIM ** (-0.5),
                project(grad_scores, query),
                project(lowered(chance), grads),
            )
        )
    first = head_lanes(0)
    for index, out_ref in enumerate((dq_ref, dk_ref, dv_ref)):
        out_ref[...] = lowered(jnp.where(first, parts[0][index], parts[1][index]))


def attend_back(lengths, qk, values, grads, seq, sources=(), scatter=None, collective=None):
    rows, width = values.shape
    pairs = width // PAIR
    flops = 10 * rows * seq * width
    spec = pl.BlockSpec((seq, PAIR), lambda s, h, n: (s, h))
    shape = jax.ShapeDtypeStruct((rows, width), jnp.bfloat16)
    body, more_in, more_out, more_shape, scratch, params = attend_back_kernel, [], [], [], [], None
    if scatter is not None:
        body = carried(
            attend_back_kernel,
            scatter,
            4,
            3,
            1,
            rows // seq * pairs,
            2.7,
            lambda: pl.program_id(0) * pairs + pl.program_id(1),
        )
        more_in, more_out, more_shape = scatter.in_specs(), scatter.out_specs(), scatter.out_shape()
        scratch = scatter.scratch()
        params = pltpu.CompilerParams(
            collective_id=collective, has_side_effects=True, vmem_limit_bytes=VMEM_BYTES
        )
    result = pl.pallas_call(
        body,
        grid_spec=pltpu.PrefetchScalarGridSpec(
            num_scalar_prefetch=1,
            grid=(rows // seq, pairs),
            in_specs=[
                spec,
                pl.BlockSpec((seq, PAIR), lambda s, h, n: (s, pairs + h)),
                spec,
                spec,
            ]
            + more_in,
            out_specs=[spec, spec, spec] + more_out,
            scratch_shapes=scratch,
        ),
        out_shape=[shape, shape, shape] + more_shape,
        compiler_params=params,
        cost_estimate=pl.CostEstimate(
            flops=8 * flops, bytes_accessed=14 * rows * width, transcendentals=rows * seq * 12
        ),
        name="attend_back",
    )(lengths, qk, qk, values, grads, *sources)
    return result[:3], result[3:]


def expand_kernel(h_ref, w_ref, b_ref, u_ref, slope_ref):
    inner = project(h_ref[...], w_ref[...]) + b_ref[...]
    bell = jnp.exp(inner * inner * -0.5)
    step = 1.0 / (1.0 + TAIL_P * jnp.abs(inner))
    poly = jnp.full_like(step, TAIL_C[-1])
    for coefficient in reversed(TAIL_C[:-1]):
        poly = poly * step + coefficient
    tail = poly * step * bell
    below = jnp.where(inner >= 0, 1.0 - tail, tail)
    u_ref[...] = lowered(inner * below)
    slope_ref[...] = lowered(below + inner * bell * INV_SQRT_2PI)


def expand(normed, weight, bias, shards=(), gather=None, collective=None, tile=256):
    rows, width = normed.shape
    hidden = weight.shape[1]
    body, more_in, more_out, more_shape, scratch, params = expand_kernel, [], [], [], [], None
    aliases = {}
    if gather is not None:
        body = carried(
            expand_kernel, gather, 3, 2, 0, hidden // tile, 1.6, lambda: pl.program_id(0)
        )
        more_in, more_out, more_shape = gather.in_specs(), gather.out_specs(), gather.out_shape()
        scratch, aliases = gather.scratch(), gather.aliases(3, 2)
        params = pltpu.CompilerParams(collective_id=collective, has_side_effects=True)
    shape = jax.ShapeDtypeStruct((rows, hidden), jnp.bfloat16)
    out_spec = pl.BlockSpec((rows, tile), lambda j: (0, j))
    result = pl.pallas_call(
        body,
        grid=(hidden // tile,),
        in_specs=[
            pl.BlockSpec((rows, width), lambda j: (0, 0)),
            pl.BlockSpec((width, tile), lambda j: (0, j)),
            pl.BlockSpec((1, tile), lambda j: (0, j)),
        ]
        + more_in,
        out_specs=[out_spec, out_spec] + more_out,
        out_shape=[shape, shape] + more_shape,
        scratch_shapes=scratch,
        input_output_aliases=aliases,
        compiler_params=params,
        cost_estimate=pl.CostEstimate(
            flops=6 * rows * width * hidden,
            bytes_accessed=2 * width * hidden + 4 * rows * hidden,
            transcendentals=2 * rows * hidden,
        ),
        name="expand",
    )(normed, weight, bias, *shards)
    return result[0], result[1], result[2:]


def norm_parts(value):
    centred = value - jnp.mean(value, axis=-1, keepdims=True)
    inverse = lax.rsqrt(jnp.mean(centred * centred, axis=-1, keepdims=True) + NORM_EPS)
    return centred * inverse, inverse


def norm_back(grad, value, gain):
    unit, inverse = norm_parts(value)
    grad_gain = jnp.sum(grad * unit, axis=0)
    grad_shift = jnp.sum(grad, axis=0)
    grad_unit = grad * gain
    grad_value = inverse * (
        grad_unit
        - jnp.mean(grad_unit, axis=-1, keepdims=True)
        - unit * jnp.mean(grad_unit * unit, axis=-1, keepdims=True)
    )
    return grad_value, grad_gain, grad_shift


class Weights:
    def __init__(self, w_qk, w_vo, spread):
        width = spread.shape[0]
        self.w_qk, self.w_vo = w_qk, w_vo
        place = w_vo[:, 2 * width :]
        self.vec_plain = jnp.transpose(project(spread, place))
        self.vec_place = jnp.transpose(place.astype(jnp.float32))
        self.w_up = self.w_down = None


def layer_ahead(rows, weights, lengths, seq, during_attend, during_expand):
    width = rows.shape[1]
    plain, vec_place = weights.vec_plain, weights.vec_place
    bias_q, bias_v, bias_up = plain[0], plain[1], plain[8:12].reshape(1, -1)
    bias_qk = jnp.concatenate([bias_q, jnp.zeros_like(bias_q)])
    qk = lowered(project(rows, weights.w_qk) + bias_qk)
    values = lowered(project(rows, weights.w_vo[:, :width]) + bias_v)
    context = during_attend(lengths, qk, values, seq)
    first_sum = (
        rows.astype(jnp.float32)
        + project_back(context, weights.w_vo[:, width : 2 * width])
        + vec_place[2]
    )
    normed = lowered(norm_parts(first_sum)[0] * vec_place[3] + vec_place[4])
    active, slope = during_expand(normed, bias_up)
    second_sum = normed.astype(jnp.float32) + project_back(active, weights.w_down) + vec_place[7]
    output = lowered(norm_parts(second_sum)[0] * vec_place[5] + vec_place[6])
    return output, (qk, values, context, first_sum, normed, active, slope, second_sum)


def layer_behind(grad_out, rows, kept, weights, spread, give, during_attend):
    w_qk, w_vo, w_up, w_down = weights.w_qk, weights.w_vo, weights.w_up, weights.w_down
    vec_place = weights.vec_place
    width = rows.shape[1]
    qk, values, context, first_sum, normed, active, slope, second_sum = kept
    grad_second, gain_two, shift_two = norm_back(grad_out, second_sum, vec_place[5])
    grad_ffn = lowered(grad_second)
    bias_out = jnp.sum(grad_ffn.astype(jnp.float32), axis=0)
    give("down", grad_ffn, active)
    grad_inner = lowered(project(grad_ffn, w_down) * slope.astype(jnp.float32))
    bias_inner = jnp.sum(grad_inner.astype(jnp.float32), axis=0)
    give("up", normed, grad_inner)
    grad_normed = grad_second + project_back(grad_inner, w_up)
    grad_first, gain_one, shift_one = norm_back(grad_normed, first_sum, vec_place[3])
    grad_attn = lowered(grad_first)
    bias_attn = jnp.sum(grad_attn.astype(jnp.float32), axis=0)
    give("out", grad_attn, context)
    grad_context = lowered(project(grad_attn, w_vo[:, width : 2 * width]))
    grad_query, grad_keys, grad_values = during_attend(qk, values, grad_context)
    bias_query = jnp.sum(grad_query.astype(jnp.float32), axis=0)
    bias_value = jnp.sum(grad_values.astype(jnp.float32), axis=0)
    give("value", rows, grad_values)
    give("query", rows, grad_query)
    give("key", rows, grad_keys)
    grad_rows = grad_first + project_back(grad_query, w_qk[:, :width])
    grad_rows = grad_rows + project_back(grad_keys, w_qk[:, width:])
    grad_rows = grad_rows + project_back(grad_values, w_vo[:, :width])
    plain = jnp.concatenate(
        [jnp.stack([bias_query, bias_value]), bias_inner.reshape(-1, width)], axis=0
    )
    placed = jnp.dot(plain, spread.astype(jnp.float32), precision=lax.Precision.HIGHEST)
    vec_grad = jnp.stack(
        [
            placed[0],
            placed[1],
            bias_attn,
            gain_one,
            shift_one,
            gain_two,
            shift_two,
            bias_out,
            placed[2],
            placed[3],
            placed[4],
            placed[5],
        ],
        axis=1,
    )
    return grad_rows, vec_grad


ATTN_NAMES = ("query", "key", "value", "out")
FFN_NAMES = ("up", "down")
FLIPPED = ("value", "out", "down")


def behind_permuted(grad_rows, layer_inputs, kept_all, weights_all, lengths, seq, spread):
    summed, vec_all = {}, {}
    for layer in reversed(range(len(kept_all))):

        def give(name, left, right):
            summed[layer, name] = outer_scatter(left, right, name in FLIPPED)

        def during_attend(qk, values, grads):
            return attend_back(lengths, qk, values, grads, seq)[0]

        grad_rows, vec_all[layer] = layer_behind(
            grad_rows,
            layer_inputs[layer],
            kept_all[layer],
            weights_all[layer],
            spread,
            give,
            during_attend,
        )
    vec_local = jnp.concatenate([vec_all[layer] for layer in sorted(vec_all)], axis=1)
    half = vec_local.shape[0] // 2
    vec_sum = scatter_rows(vec_local[:half], vec_local[half:], False, jnp.float32)
    return grad_rows, summed, vec_sum


def behind_carried(grad_rows, layer_inputs, kept_all, weights_all, lengths, seq, spread):
    width = spread.shape[0]
    layers = len(kept_all)
    products, eighths, summed, vec_all = {}, {}, {}, {}

    def plan(wanted):
        sources, arrays = [], []
        for layer, name, span in wanted:
            source = eighths[layer, name] if span == "back" else products[layer, name]
            sources.append(source)
            columns = source.shape[1]
            parts = 4 if columns > width else 2 if columns == width else 1
            arrays.append((columns, source.dtype, span, parts, int(name in FLIPPED)))

        def keep(results):
            for (layer, name, span), result in zip(wanted, results):
                (eighths if span == "front" else summed)[layer, name] = result

        return sources, Scatter(arrays).set_rows(width), keep

    for layer in reversed(range(layers)):

        def give(name, left, right):
            products[layer, name] = lowered(outer_sum(left, right))

        def during_attend(qk, values, grads):
            wanted = [(layer, name, "front") for name in FFN_NAMES]
            if layer + 1 < layers:
                wanted = [(layer + 1, name, "back") for name in FFN_NAMES] + wanted
                wanted += [(layer + 1, name, "full") for name in ATTN_NAMES]
            sources, scatter, keep = plan(wanted)
            grads_qkv, arrived = attend_back(
                lengths, qk, values, grads, seq, sources, scatter, 16 + layer
            )
            keep(arrived)
            return grads_qkv

        grad_rows, vec_all[layer] = layer_behind(
            grad_rows,
            layer_inputs[layer],
            kept_all[layer],
            weights_all[layer],
            spread,
            give,
            during_attend,
        )
    vec_local = jnp.concatenate([vec_all[layer] for layer in range(layers)], axis=1)
    vec_columns = vec_local.shape[1]
    products[0, "vec"] = jnp.pad(vec_local, ((0, 0), (0, 128 - vec_columns)))
    sources, scatter, keep = plan(
        [(0, name, "full") for name in ATTN_NAMES]
        + [(0, "vec", "full")]
        + [(0, name, "back") for name in FFN_NAMES]
    )
    keep(scatter_alone(scatter, sources, 15))
    return grad_rows, summed, summed[0, "vec"][:, :vec_columns]


def ahead_permuted(rows, shards_all, spread, lengths, seq):
    layer_inputs, kept_all, weights_all = [], [], []
    for shards in shards_all:
        weights = Weights(gather_rows(shards[0], False), gather_rows(shards[1], True), spread)
        weights.w_up = gather_rows(shards[2], False)
        weights.w_down = gather_rows(shards[3], True)
        layer_inputs.append(rows)
        rows, kept = layer_ahead(
            rows,
            weights,
            lengths,
            seq,
            lambda *operands: attend(*operands)[0],
            lambda normed, bias, weights=weights: expand(normed, weights.w_up, bias)[:2],
        )
        kept_all.append(kept)
        weights_all.append(weights)
    return rows, layer_inputs, kept_all, weights_all


def ahead_carried(rows, shards_all, spread, lengths, seq):
    devices = lax.axis_size("dp")
    bits = bit_count(devices)
    layers = len(shards_all)

    along = 2
    last = bits - 1
    arrays = {}

    def plan(*wanted):
        wanted = [item for item in wanted if item[0] < layers]
        operands, shapes = [], []
        for layer, index, first, _ in wanted:
            shard = shards_all[layer][index][None]
            operands.append(arrays[layer, index] if first else shard)
            shapes.append((devices,) + shard.shape[1:])
        spans = [item[2:] for item in wanted]
        flips = [item[1] % 2 for item in wanted]

        def keep(results):
            for (layer, index, _, _), result in zip(wanted, results):
                arrays[layer, index] = result

        return operands, Gather(shapes, spans, flips, bits), keep

    def flat(layer, index):
        array = arrays[layer, index]
        return array.reshape(-1, array.shape[2])

    operands, gather, keep = plan((0, 0, 0, last), (0, 1, 0, last), (0, 2, 0, along - 1), (1, 0, 0, along - 1))
    keep(gather_alone(gather, operands, 0))
    layer_inputs, kept_all, weights_all = [], [], []
    for layer in range(layers):
        weights = Weights(flat(layer, 0), flat(layer, 1), spread)

        def during_attend(lengths, qk, values, seq):
            operands, gather, keep = plan(
                (layer, 2, along, last),
                (layer + 1, 0, along, last),
                (layer, 3, 0, along - 1),
                (layer + 1, 1, 0, along - 1),
            )
            context, arrived = attend(
                lengths, qk, values, seq, operands, gather, 1 + 2 * layer
            )
            keep(arrived)
            weights.w_up = flat(layer, 2)
            return context

        def during_expand(normed, bias):
            operands, gather, keep = plan(
                (layer, 3, along, last),
                (layer + 1, 1, along, last),
                (layer + 1, 2, 0, along - 1),
                (layer + 2, 0, 0, along - 1),
            )
            active, slope, arrived = expand(
                normed, weights.w_up, bias, operands, gather, 2 + 2 * layer
            )
            keep(arrived)
            weights.w_down = flat(layer, 3)
            return active, slope

        layer_inputs.append(rows)
        rows, kept = layer_ahead(rows, weights, lengths, seq, during_attend, during_expand)
        kept_all.append(kept)
        weights_all.append(weights)
    return rows, layer_inputs, kept_all, weights_all


def adam_step(param, first, second, grad):
    first_new = 0.9 * first + 0.1 * grad
    second_new = 0.98 * second + 0.02 * grad * grad
    first_hat = first_new / (1.0 - 0.9**10)
    second_hat = second_new / (1.0 - 0.98**10)
    direction = first_hat / (jnp.sqrt(second_hat) + 1e-08) + 0.01 * param
    return (direction, first_new, second_new)


def local(
    tokens,
    cotangent,
    lengths,
    counts,
    attn_w,
    ffn_w,
    vec_w,
    attn_m,
    ffn_m,
    vec_m,
    attn_v,
    ffn_v,
    vec_v,
):
    row_total, width = tokens.shape
    seq = row_total // lengths.shape[0]
    layers = attn_w.shape[0]
    hidden = ffn_w.shape[2] // 2
    vec_rows = vec_w.shape[1]
    micro = lax.broadcasted_iota(jnp.int32, (row_total, 1), 0) // (seq * SEQ_MB)
    live = micro < counts[0]
    spread = order_matrix(width)
    shards_all = []
    for layer in range(layers):
        attn = lowered(attn_w[layer])
        ffn = lowered(ffn_w[layer])
        vec = jnp.pad(jnp.transpose(lowered(vec_w[layer])), ((0, 0), (0, 128 - vec_rows)))
        shards_all.append(
            (
                attn[:, : 2 * width],
                jnp.concatenate([attn[:, 2 * width :], vec], axis=1),
                ffn[:, :hidden],
                ffn[:, hidden:],
            )
        )
    carry = lax.axis_size("dp") == 32 and attn_w.shape[1] % 8 == 0
    ahead = ahead_carried if carry else ahead_permuted
    behind = behind_carried if carry else behind_permuted
    rows = lowered(project(tokens, spread))
    rows, layer_inputs, kept_all, weights_all = ahead(rows, shards_all, spread, lengths, seq)
    activations = lowered(jnp.where(live, project_back(rows, spread), 0.0))
    grad_rows = jnp.where(live, project(cotangent, spread), 0.0)
    grad_rows, summed, vec_sum = behind(
        grad_rows, layer_inputs, kept_all, weights_all, lengths, seq, spread
    )
    high = lax.reduce_precision(grad_rows, 8, 7)
    in_grad = project_back(lowered(high), spread) + project_back(lowered(grad_rows - high), spread)
    vec_sum = jnp.transpose(vec_sum).reshape(layers, vec_rows, -1)
    factor = float(row_total * lax.axis_size("dp")) ** (-0.5)

    def joined(names):
        return jnp.stack(
            [
                jnp.concatenate([summed[layer, name] for name in names], axis=1)
                for layer in range(layers)
            ]
        )

    attn_grad = joined(ATTN_NAMES) * factor
    ffn_grad = joined(FFN_NAMES) * factor
    vec_grad = vec_sum * factor
    attn_step, attn_m_new, attn_v_new = adam_step(attn_w, attn_m, attn_v, attn_grad)
    ffn_step, ffn_m_new, ffn_v_new = adam_step(ffn_w, ffn_m, ffn_v, ffn_grad)
    vec_step, vec_m_new, vec_v_new = adam_step(vec_w, vec_m, vec_v, vec_grad)
    return (
        activations,
        in_grad,
        attn_grad,
        ffn_grad,
        vec_grad,
        attn_step,
        ffn_step,
        vec_step,
        attn_m_new,
        ffn_m_new,
        vec_m_new,
        attn_v_new,
        ffn_v_new,
        vec_v_new,
    )


def solution(mesh):
    rows = P("dp", None)
    weight = P(None, "dp", None)
    vector = P(None, None, "dp")
    in_specs = (rows, rows, P("dp"), P("dp")) + (weight, weight, vector) * 3
    out_specs = (rows, rows) + (weight, weight, vector) * 4
    return jax.shard_map(local, mesh=mesh, in_specs=in_specs, out_specs=out_specs, check_vma=False)
```

```python
import functools

import jax
import jax.numpy as jnp
from jax import lax
from jax.experimental import pallas as pl
from jax.experimental.pallas import tpu as pltpu
from jax.sharding import PartitionSpec as P

HEAD_DIM = 64
SEQ_MB = 1
PAIR = 2 * HEAD_DIM

NORM_EPS = 1e-05
MASK_VALUE = -1e30

TAIL_P = 0.275
TAIL_C = (0.1178092576, 0.04211145346, 0.3339323636, -0.3309935012, 0.4519987806, -0.1148583494)
INV_SQRT_2PI = 0.3989422804014327


def lowered(value):
    return value.astype(jnp.bfloat16)


def project(left, right):
    return jnp.dot(left, right, preferred_element_type=jnp.float32)


def project_back(left, right):
    return lax.dot_general(
        left, right, (((1,), (1,)), ((), ())), preferred_element_type=jnp.float32
    )


def outer_sum(left, right):
    return lax.dot_general(
        left, right, (((0,), (0,)), ((), ())), preferred_element_type=jnp.float32
    )


def bit_count(devices):
    bits = devices.bit_length() - 1
    assert 1 << bits == devices
    return bits


def swap(value, bit):
    devices = lax.axis_size("dp")
    return lax.ppermute(value, "dp", [(i, i ^ (1 << bit)) for i in range(devices)])


def gather_rows(shard, flip):
    bits = bit_count(lax.axis_size("dp"))
    rows = shard
    for bit in reversed(range(3 if flip else 0, bits)):
        rows = jnp.concatenate([rows, swap(rows, bit)], axis=0)
    if flip:
        height, width = rows.shape
        rows = jnp.concatenate([rows[None], swap(rows, 1)[None]], axis=0)
        rows = jnp.concatenate([rows[:, None], swap(rows, 2)[:, None]], axis=1)
        rows = rows.reshape(4 * height, width)
        rows = jnp.concatenate([rows, swap(rows, 0)], axis=0)
    return rows


def scatter_rows(keep, send, flip, wire):
    bits = bit_count(lax.axis_size("dp"))
    total = keep + swap(send.astype(wire), 0).astype(jnp.float32)
    start = 1
    if flip:
        total = total.astype(wire)
        height, width = total.shape
        quarter = total.reshape(2, 2, height // 4, width)
        total = quarter[:, 0].astype(jnp.float32) + swap(quarter[:, 1], 2).astype(jnp.float32)
        total = total.astype(wire)
        total = total[0].astype(jnp.float32) + swap(total[1], 1).astype(jnp.float32)
        start = 3
    for bit in range(start, bits):
        total = total.astype(wire)
        half = total.shape[0] // 2
        total = total[:half].astype(jnp.float32) + swap(total[half:], bit).astype(jnp.float32)
    return total


def order_matrix(width):
    devices = lax.axis_size("dp")
    bits = bit_count(devices)
    block = width // devices
    place = lax.broadcasted_iota(jnp.int32, (width, width), 1)
    feature = lax.broadcasted_iota(jnp.int32, (width, width), 0)
    part = place // block
    mirrored = jnp.zeros_like(part)
    for bit in range(bits):
        mirrored = mirrored | (((part >> bit) & 1) << (bits - 1 - bit))
    wanted = (mirrored ^ lax.axis_index("dp")) * block + place % block
    return (feature == wanted).astype(jnp.bfloat16)


LINK_BYTES_US = 90e3
CORE_BYTES_US = 900e3
HOP_US = 1.5
PARTS = 6
VMEM_BYTES = 40 << 20


class Gather:
    def __init__(self, shapes, spans, delays, flips, bits):
        self.delays = delays
        self.shapes = shapes
        self.ins = self.outs = len(shapes)
        self.spans = spans
        self.bits = bits
        self.pieces = []
        self.steps = []
        for array, (shape, flip_first) in enumerate(zip(shapes, flips)):
            lanes = shape[2] // 128
            edges = [128 * (lanes * part // PARTS) for part in range(PARTS + 1)]
            for part in range(PARTS):
                flip = (part + flip_first) % 2 == 1
                self.pieces.append((array, edges[part], edges[part + 1] - edges[part], flip))
                self.steps.append(self.plan(flip))
        self.slots = {}
        for piece, plan in enumerate(self.steps):
            first, last = spans[self.pieces[piece][0]]
            for step in range(first, last + 1):
                for run in range(len(plan[step][1])):
                    self.slots[piece, step, run] = len(self.slots)

    def plan(self, flip):
        order = list(reversed(range(self.bits)))
        if flip:
            order[self.bits - 3], order[self.bits - 2] = 1, 2
        held = [0]
        plan = []
        for bit in order:
            offset = 1 << (self.bits - 1 - bit)
            runs = []
            for block in held:
                if runs and runs[-1][0] + runs[-1][1] == block:
                    runs[-1][1] += 1
                else:
                    runs.append([block, 1])
            plan.append((bit, [(first, count, first + offset) for first, count in runs]))
            held = sorted(held + [block + offset for block in held])
        return plan

    def timetable(self):
        free = {}
        ready = {
            array: (delay, array, span[0])
            for array, (span, delay) in enumerate(zip(self.spans, self.delays))
        }
        events = []
        while ready:
            time, array, step = min(ready.values())
            done = time
            for piece, (owner, _, columns, _) in enumerate(self.pieces):
                if owner != array:
                    continue
                bit, runs = self.steps[piece][step]
                link = min(bit, 3)
                size = sum(count for _, count, _ in runs) * self.shapes[array][1] * columns * 2
                if bit == 0:
                    span = size / CORE_BYTES_US
                else:
                    span = size * (4 if bit == 4 else 2) / LINK_BYTES_US
                events.append((time, piece, step))
                free[link] = max(time, free.get(link, 0.0)) + span
                done = max(done, free[link])
            if step == self.spans[array][1]:
                del ready[array]
            else:
                ready[array] = (done + HOP_US, array, step + 1)
        return events

    def scratch(self):
        count = len(self.slots)
        return [
            pltpu.SemaphoreType.DMA((count,)),
            pltpu.SemaphoreType.DMA((count,)),
            pltpu.SemaphoreType.DMA((len(self.pieces),)),
        ]

    def in_specs(self):
        return [
            pl.BlockSpec(memory_space=pl.ANY if span[0] else pltpu.VMEM) for span in self.spans
        ]

    def out_specs(self):
        return [pl.BlockSpec(memory_space=pl.ANY)] * len(self.shapes)

    def out_shape(self):
        return [jax.ShapeDtypeStruct(shape, jnp.bfloat16) for shape in self.shapes]

    def aliases(self, inputs, outputs):
        return {
            inputs + array: outputs + array for array, span in enumerate(self.spans) if span[0]
        }

    def bind(self, shards, dests, sems):
        self.shards, self.dests = shards, dests
        self.send_sem, self.recv_sem, self.own_sem = sems

    def partner(self, bit):
        me = lax.axis_index("dp")
        return me + (1 << bit) * (1 - 2 * ((me // (1 << bit)) % 2))

    def copies(self, piece, step):
        array, start, columns, _ = self.pieces[piece]
        bit, runs = self.steps[piece][step]
        dest = self.dests[array]
        lanes = pl.ds(start, columns)
        made = []
        for run, (first, count, target) in enumerate(runs):
            slot = self.slots[piece, step, run]
            if step == 0:
                source = self.shards[array].at[:, :, lanes]
            else:
                source = dest.at[pl.ds(first, count), :, lanes]
            made.append(
                pltpu.make_async_remote_copy(
                    src_ref=source,
                    dst_ref=dest.at[pl.ds(target, count), :, lanes],
                    send_sem=self.send_sem.at[slot],
                    recv_sem=self.recv_sem.at[slot],
                    device_id=(self.partner(bit),),
                    device_id_type=pl.DeviceIdType.MESH,
                )
            )
        return made

    def own(self, piece):
        array, start, columns, _ = self.pieces[piece]
        lanes = pl.ds(start, columns)
        return pltpu.make_async_copy(
            self.shards[array].at[:, :, lanes],
            self.dests[array].at[pl.ds(0, 1), :, lanes],
            self.own_sem.at[piece],
        )

    def begin(self):
        barrier = pltpu.get_barrier_semaphore()
        for bit in range(self.bits):
            pl.semaphore_signal(
                barrier,
                inc=1,
                device_id=(self.partner(bit),),
                device_id_type=pl.DeviceIdType.MESH,
            )
        pl.semaphore_wait(barrier, self.bits)
        for piece in range(len(self.pieces)):
            if self.first(piece) == 0:
                self.own(piece).start()

    def first(self, piece):
        return self.spans[self.pieces[piece][0]][0]

    def last(self, piece):
        return self.spans[self.pieces[piece][0]][1]

    def advance(self, piece, step):
        if step == 1 and self.first(piece) == 0:
            self.own(piece).wait()
        if step > self.first(piece):
            for copy in self.copies(piece, step - 1):
                copy.wait_recv()
        for copy in self.copies(piece, step):
            copy.start()

    def finish(self):
        for piece in range(len(self.pieces)):
            for copy in self.copies(piece, self.last(piece)):
                copy.wait_recv()
        for piece in range(len(self.pieces)):
            for step in range(self.first(piece), self.last(piece) + 1):
                for copy in self.copies(piece, step):
                    copy.wait_send()


class Scatter:
    def __init__(self, arrays, places, results, rows):
        self.given = arrays
        self.places = places
        self.made = results
        self.rows = rows
        self.arrays = self.ins = len(arrays)
        self.outs = len(results)
        self.pieces = []
        for array, (columns, _, _, parts, first) in enumerate(arrays):
            lanes = columns // 128
            edges = [128 * (lanes * part // parts) for part in range(parts + 1)]
            for part in range(parts):
                flip = (part + first) % 2
                self.pieces.append((array, edges[part], edges[part + 1] - edges[part], flip))

    def range_of(self, array):
        return {"full": (0, 4), "front": (0, 2), "back": (3, 4)}[self.given[array][2]]

    def link(self, step, flip):
        return (0, 2, 1, 3, 4)[step] if flip else (0, 1, 2, 3, 4)[step]

    def timetable(self):
        free = {}
        ready = {array: (0.0, array, self.range_of(array)[0]) for array in range(self.arrays)}
        events = []
        while ready:
            time, array, step = min(ready.values())
            done = time
            last = self.range_of(array)[1]
            for piece, (owner, _, columns, flip) in enumerate(self.pieces):
                if owner != array:
                    continue
                events.append((time, piece, step))
                if step > last:
                    continue
                bit = self.link(step, flip)
                size = (self.rows >> (step + 1)) * columns * jnp.dtype(self.given[array][1]).itemsize
                if bit == 0:
                    span = size / CORE_BYTES_US
                else:
                    span = size * (4 if bit == 4 else 2) / LINK_BYTES_US
                link = min(bit, 3)
                free[link] = max(time, free.get(link, 0.0)) + span
                done = max(done, free[link])
            if step > last:
                del ready[array]
            else:
                ready[array] = (done + HOP_US, array, step + 1)
        return events

    def in_specs(self):
        return [
            pl.BlockSpec(memory_space=pltpu.VMEM if given[2] == "back" else pl.ANY)
            for given in self.given
        ]

    def out_specs(self):
        return [pl.BlockSpec(memory_space=pltpu.VMEM)] * self.outs

    def out_shape(self):
        return self.made

    def aliases(self, inputs, outputs):
        return {}

    def scratch(self):
        made = []
        for columns, kind, span, _, _ in self.given:
            if span != "back":
                made += [pltpu.VMEM((self.rows // 2, columns), kind)] * 2
                made.append(pltpu.VMEM((self.rows // 4, columns), kind))
                made.append(pltpu.VMEM((self.rows // 8, columns), kind))
            if span != "front":
                made.append(pltpu.VMEM((self.rows // 16, columns), kind))
                made += [pltpu.VMEM((self.rows // 32, columns), kind)] * 2
                made.append(pltpu.VMEM((self.rows // 32, columns), jnp.float32))
        count = len(self.pieces)
        made += [pltpu.SemaphoreType.DMA((count * 6,))] * 2
        made.append(pltpu.SemaphoreType.DMA((count,)))
        return made

    def bind(self, sources, results, scratch):
        self.sources, self.results = sources, results
        scratch = list(scratch)
        self.part, self.landing, self.leaving, self.own = {}, {}, {}, {}
        for array, given in enumerate(self.given):
            if given[2] != "back":
                self.part[array], self.landing[array, 0] = scratch.pop(0), scratch.pop(0)
                self.landing[array, 1], self.landing[array, 2] = scratch.pop(0), scratch.pop(0)
            else:
                self.part[array] = sources[array]
            if given[2] != "front":
                self.landing[array, 3] = scratch.pop(0)
                self.landing[array, 4], self.leaving[array] = scratch.pop(0), scratch.pop(0)
                self.own[array] = scratch.pop(0)
        self.send_sem, self.recv_sem, self.own_sem = scratch

    def partner(self, bit):
        me = lax.axis_index("dp")
        return me + (1 << bit) * (1 - 2 * ((me // (1 << bit)) % 2))

    def begin(self):
        barrier = pltpu.get_barrier_semaphore()
        for bit in range(5):
            pl.semaphore_signal(
                barrier,
                inc=1,
                device_id=(self.partner(bit),),
                device_id_type=pl.DeviceIdType.MESH,
            )
        pl.semaphore_wait(barrier, 5)

    def fetch(self, piece):
        array, start, columns, _ = self.pieces[piece]
        lanes = pl.ds(start, columns)
        half = self.rows // 2
        return pltpu.make_async_copy(
            self.sources[array].at[pl.ds(0, half), lanes],
            self.part[array].at[:, lanes],
            self.own_sem.at[piece],
        )

    def copies(self, piece, step):
        array, start, columns, flip = self.pieces[piece]
        lanes = pl.ds(start, columns)
        size = self.rows >> (step + 1)
        source = self.part[array]
        if step == 0:
            source, runs = self.sources[array], [(size, 0, size)]
        elif step == 1 and flip:
            runs = [(size // 2, 0, size // 2), (3 * size // 2, size // 2, size // 2)]
        elif step == 4:
            source, runs = self.leaving[array], [(0, 0, size)]
        elif step == 2 and flip:
            runs = [(2 * size, 0, size)]
        else:
            runs = [(size, 0, size)]
        made = []
        for run, (first, target, count) in enumerate(runs):
            slot = piece * 6 + (step if run == 0 else 5)
            made.append(
                pltpu.make_async_remote_copy(
                    src_ref=source.at[pl.ds(first, count), lanes],
                    dst_ref=self.landing[array, step].at[pl.ds(target, count), lanes],
                    send_sem=self.send_sem.at[slot],
                    recv_sem=self.recv_sem.at[slot],
                    device_id=(self.partner(self.link(step, flip)),),
                    device_id_type=pl.DeviceIdType.MESH,
                )
            )
        return made

    def add(self, piece, step):
        array, start, columns, flip = self.pieces[piece]
        lanes = pl.ds(start, columns)
        part, landed = self.part[array], self.landing[array, step]
        size = self.rows >> (step + 1)
        if step == 4:
            result, offset = self.places[array]
            self.results[result][:, pl.ds(offset + start, columns)] = self.own[array][
                :, lanes
            ] + landed[:, lanes].astype(jnp.float32)
        elif step == 3:
            total = part[pl.ds(0, size), lanes].astype(jnp.float32) + landed[:, lanes].astype(
                jnp.float32
            )
            self.own[array][:, lanes] = total[: size // 2]
            self.leaving[array][:, lanes] = total[size // 2 :].astype(self.given[array][1])
        elif step == 2 and self.given[array][2] == "front":
            result = self.places[array][0]
            self.results[result][:, lanes] = part[pl.ds(0, size), lanes] + landed[:, lanes]
        else:
            block = self.rows // 16
            skip = size // 2 if step == 1 and flip else None

            def body(index, carry):
                from_row = pl.multiple_of(index * block, block)
                row = from_row
                if skip:
                    row = pl.multiple_of(from_row + (index // (skip // block)) * skip, block)
                part[pl.ds(row, block), lanes] = (
                    part[pl.ds(row, block), lanes] + landed[pl.ds(from_row, block), lanes]
                )
                return carry

            lax.fori_loop(0, size // block, body, 0)

    def advance(self, piece, step):
        first, last = self.range_of(self.pieces[piece][0])
        if step == 0:
            self.fetch(piece).start()
        if step > first:
            if step == 1:
                self.fetch(piece).wait()
            for copy in self.copies(piece, step - 1):
                copy.wait_recv()
            self.add(piece, step - 1)
        if step <= last:
            for copy in self.copies(piece, step):
                copy.start()

    def finish(self):
        for piece in range(len(self.pieces)):
            first, last = self.range_of(self.pieces[piece][0])
            for step in range(first, last + 1):
                for copy in self.copies(piece, step):
                    copy.wait_send()


def carried(body, gather, inputs, outputs, prefetch, steps, step_us, place):
    ins, outs = gather.ins, gather.outs
    agenda = [[] for _ in range(steps)]
    for time, piece, step in gather.timetable():
        agenda[min(steps - 1, int(-(-time // step_us)))].append((piece, step))

    def kernel(*refs):
        refs = list(refs)
        cut = prefetch + inputs
        ahead, refs = refs[:cut], refs[cut:]
        shards, refs = refs[:ins], refs[ins:]
        results, refs = refs[:outputs], refs[outputs:]
        dests, sems = refs[:outs], refs[outs:]
        gather.bind(shards, dests, sems)
        here = place()
        for index, moves in enumerate(agenda):
            if index and not moves:
                continue

            @pl.when(here == index)
            def _(index=index, moves=moves):
                if index == 0:
                    gather.begin()
                for piece, step in moves:
                    gather.advance(piece, step)

        body(*ahead, *results)

        @pl.when(here == steps - 1)
        def _():
            gather.finish()

    return kernel


def gather_kernel(gather, arrays, *refs):
    gather.bind(refs[:arrays], refs[arrays : 2 * arrays], refs[2 * arrays :])
    gather.begin()
    for _, piece, step in gather.timetable():
        gather.advance(piece, step)
    gather.finish()


def gather_alone(gather, shards, collective):
    return pl.pallas_call(
        functools.partial(gather_kernel, gather, len(shards)),
        in_specs=gather.in_specs(),
        out_specs=gather.out_specs(),
        out_shape=gather.out_shape(),
        scratch_shapes=gather.scratch(),
        input_output_aliases=gather.aliases(0, 0),
        compiler_params=pltpu.CompilerParams(collective_id=collective, has_side_effects=True),
        name="gather",
    )(*shards)


def head_lanes(which):
    return lax.broadcasted_iota(jnp.int32, (1, PAIR), 1) // HEAD_DIM == which


def carrier(body, exchange, inputs, outputs, prefetch, steps, step_us, place, collective):
    if exchange is None:
        return body, [], [], [], [], {}, pltpu.CompilerParams(vmem_limit_bytes=VMEM_BYTES)
    return (
        carried(body, exchange, inputs, outputs, prefetch, steps, step_us, place),
        exchange.in_specs(),
        exchange.out_specs(),
        exchange.out_shape(),
        exchange.scratch(),
        exchange.aliases(prefetch + inputs, outputs),
        pltpu.CompilerParams(
            collective_id=collective, has_side_effects=True, vmem_limit_bytes=VMEM_BYTES
        ),
    )


def attend_kernel(len_ref, q_ref, k_ref, v_ref, ctx_ref):
    length = len_ref[pl.program_id(0)]
    seq = k_ref.shape[0]
    query = q_ref[...] * jnp.bfloat16(HEAD_DIM ** (-0.5))
    keys = k_ref[...]
    values = v_ref[...]
    open_keys = lax.broadcasted_iota(jnp.int32, (1, seq), 1) < length
    picked = []
    for which in range(2):
        lanes = head_lanes(which)
        scores = project_back(jnp.where(lanes, query, jnp.zeros_like(query)), keys)
        scores = jnp.where(open_keys, scores, MASK_VALUE)
        expo = jnp.exp(scores - jnp.max(scores, axis=-1, keepdims=True))
        chance = expo * (1.0 / jnp.sum(expo, axis=-1, keepdims=True))
        picked.append(project(lowered(chance), values))
    ctx_ref[...] = lowered(jnp.where(head_lanes(0), picked[0], picked[1]))


def attend(lengths, qk, values, seq, shards=(), gather=None, collective=None):
    rows, width = values.shape
    pairs = width // PAIR
    flops = 4 * rows * seq * width
    body, more_in, more_out, more_shape, scratch, params = attend_kernel, [], [], [], [], None
    aliases = {}
    if gather is not None:
        steps = rows // seq * pairs
        body = carried(
            attend_kernel,
            gather,
            3,
            1,
            1,
            steps,
            1.5,
            lambda: pl.program_id(0) * pairs + pl.program_id(1),
        )
        more_in, more_out, more_shape = gather.in_specs(), gather.out_specs(), gather.out_shape()
        scratch, aliases = gather.scratch(), gather.aliases(4, 1)
        params = pltpu.CompilerParams(collective_id=collective, has_side_effects=True)
    result = pl.pallas_call(
        body,
        grid_spec=pltpu.PrefetchScalarGridSpec(
            num_scalar_prefetch=1,
            grid=(rows // seq, pairs),
            in_specs=[
                pl.BlockSpec((seq, PAIR), lambda s, h, n: (s, h)),
                pl.BlockSpec((seq, PAIR), lambda s, h, n: (s, pairs + h)),
                pl.BlockSpec((seq, PAIR), lambda s, h, n: (s, h)),
            ]
            + more_in,
            out_specs=[pl.BlockSpec((seq, PAIR), lambda s, h, n: (s, h))] + more_out,
            scratch_shapes=scratch,
        ),
        out_shape=[jax.ShapeDtypeStruct((rows, width), jnp.bfloat16)] + more_shape,
        input_output_aliases=aliases,
        compiler_params=params,
        cost_estimate=pl.CostEstimate(
            flops=8 * flops, bytes_accessed=8 * rows * width, transcendentals=rows * seq * 12
        ),
        name="attend",
    )(lengths, qk, qk, values, *shards)
    return result[0], result[1:]


def attend_back_kernel(len_ref, q_ref, k_ref, v_ref, g_ref, dq_ref, dk_ref, dv_ref):
    length = len_ref[pl.program_id(0)]
    seq = k_ref.shape[0]
    query = q_ref[...] * jnp.bfloat16(HEAD_DIM ** (-0.5))
    keys = k_ref[...]
    values = v_ref[...]
    grads = g_ref[...]
    open_keys = lax.broadcasted_iota(jnp.int32, (seq, 1), 0) < length
    parts = []
    for which in range(2):
        lanes = head_lanes(which)
        scores = project_back(keys, jnp.where(lanes, query, jnp.zeros_like(query)))
        scores = jnp.where(open_keys, scores, MASK_VALUE)
        expo = jnp.exp(scores - jnp.max(scores, axis=0, keepdims=True))
        chance = expo * (1.0 / jnp.sum(expo, axis=0, keepdims=True))
        grad_chance = project_back(values, jnp.where(lanes, grads, jnp.zeros_like(grads)))
        weighed = jnp.sum(chance * grad_chance, axis=0, keepdims=True)
        grad_scores = lowered(chance * (grad_chance - weighed))
        parts.append(
            (
                outer_sum(grad_scores, keys) * HEAD_DIM ** (-0.5),
                project(grad_scores, query),
                project(lowered(chance), grads),
            )
        )
    first = head_lanes(0)
    for index, out_ref in enumerate((dq_ref, dk_ref, dv_ref)):
        out_ref[...] = lowered(jnp.where(first, parts[0][index], parts[1][index]))


def attend_back(lengths, qk, values, grads, seq, sources=(), scatter=None, collective=None):
    rows, width = values.shape
    pairs = width // PAIR
    flops = 10 * rows * seq * width
    spec = pl.BlockSpec((seq, PAIR), lambda s, h, n: (s, h))
    shape = jax.ShapeDtypeStruct((rows, width), jnp.bfloat16)
    body, more_in, more_out, more_shape, scratch, params = attend_back_kernel, [], [], [], [], None
    if scatter is not None:
        body = carried(
            attend_back_kernel,
            scatter,
            4,
            3,
            1,
            rows // seq * pairs,
            2.7,
            lambda: pl.program_id(0) * pairs + pl.program_id(1),
        )
        more_in, more_out, more_shape = scatter.in_specs(), scatter.out_specs(), scatter.out_shape()
        scratch = scatter.scratch()
        params = pltpu.CompilerParams(
            collective_id=collective, has_side_effects=True, vmem_limit_bytes=VMEM_BYTES
        )
    result = pl.pallas_call(
        body,
        grid_spec=pltpu.PrefetchScalarGridSpec(
            num_scalar_prefetch=1,
            grid=(rows // seq, pairs),
            in_specs=[
                spec,
                pl.BlockSpec((seq, PAIR), lambda s, h, n: (s, pairs + h)),
                spec,
                spec,
            ]
            + more_in,
            out_specs=[spec, spec, spec] + more_out,
            scratch_shapes=scratch,
        ),
        out_shape=[shape, shape, shape] + more_shape,
        compiler_params=params,
        cost_estimate=pl.CostEstimate(
            flops=8 * flops, bytes_accessed=14 * rows * width, transcendentals=rows * seq * 12
        ),
        name="attend_back",
    )(lengths, qk, qk, values, grads, *sources)
    return result[:3], result[3:]


def expand_kernel(h_ref, w_ref, b_ref, u_ref, slope_ref):
    inner = project(h_ref[...], w_ref[...]) + b_ref[...]
    bell = jnp.exp(inner * inner * -0.5)
    step = 1.0 / (1.0 + TAIL_P * jnp.abs(inner))
    poly = jnp.full_like(step, TAIL_C[-1])
    for coefficient in reversed(TAIL_C[:-1]):
        poly = poly * step + coefficient
    tail = poly * step * bell
    below = jnp.where(inner >= 0, 1.0 - tail, tail)
    u_ref[...] = lowered(inner * below)
    slope_ref[...] = lowered(below + inner * bell * INV_SQRT_2PI)


def expand(normed, weight, bias, shards=(), gather=None, collective=None, tile=256):
    rows, width = normed.shape
    hidden = weight.shape[1]
    body, more_in, more_out, more_shape, scratch, params = expand_kernel, [], [], [], [], None
    aliases = {}
    if gather is not None:
        body = carried(
            expand_kernel, gather, 3, 2, 0, hidden // tile, 1.6, lambda: pl.program_id(0)
        )
        more_in, more_out, more_shape = gather.in_specs(), gather.out_specs(), gather.out_shape()
        scratch, aliases = gather.scratch(), gather.aliases(3, 2)
        params = pltpu.CompilerParams(collective_id=collective, has_side_effects=True)
    shape = jax.ShapeDtypeStruct((rows, hidden), jnp.bfloat16)
    out_spec = pl.BlockSpec((rows, tile), lambda j: (0, j))
    result = pl.pallas_call(
        body,
        grid=(hidden // tile,),
        in_specs=[
            pl.BlockSpec((rows, width), lambda j: (0, 0)),
            pl.BlockSpec((width, tile), lambda j: (0, j)),
            pl.BlockSpec((1, tile), lambda j: (0, j)),
        ]
        + more_in,
        out_specs=[out_spec, out_spec] + more_out,
        out_shape=[shape, shape] + more_shape,
        scratch_shapes=scratch,
        input_output_aliases=aliases,
        compiler_params=params,
        cost_estimate=pl.CostEstimate(
            flops=6 * rows * width * hidden,
            bytes_accessed=2 * width * hidden + 4 * rows * hidden,
            transcendentals=2 * rows * hidden,
        ),
        name="expand",
    )(normed, weight, bias, *shards)
    return result[0], result[1], result[2:]


def enter_back_kernel(first_ref, dq_ref, dk_ref, dv_ref, qk_ref, vo_ref, spread_ref, out_ref):
    width = first_ref.shape[1]
    total = first_ref[...] + project_back(dq_ref[...], qk_ref[:, :width])
    total = total + project_back(dk_ref[...], qk_ref[:, width:])
    total = total + project_back(dv_ref[...], vo_ref[:, :width])
    high = lowered(total)
    rest = lowered(total - high.astype(jnp.float32))
    spread = spread_ref[...]
    out_ref[...] = project_back(high, spread) + project_back(rest, spread)


def enter_back(
    first, grads, w_qk, w_vo, spread, sources=(), scatter=None, collective=None, tile=256
):
    rows, width = first.shape
    body, more_in, more_out, more_shape, scratch, aliases, params = carrier(
        enter_back_kernel, scatter, 7, 1, 0, rows // tile, 3.9, lambda: pl.program_id(0), collective
    )
    block = pl.BlockSpec((tile, width), lambda i: (i, 0))

    def whole(shape):
        return pl.BlockSpec(shape, lambda i: (0, 0))

    result = pl.pallas_call(
        body,
        grid=(rows // tile,),
        in_specs=[
            block,
            block,
            block,
            block,
            whole(w_qk.shape),
            whole(w_vo.shape),
            whole(spread.shape),
        ]
        + more_in,
        out_specs=[block] + more_out,
        out_shape=[jax.ShapeDtypeStruct((rows, width), jnp.float32)] + more_shape,
        scratch_shapes=scratch,
        input_output_aliases=aliases,
        compiler_params=params,
        cost_estimate=pl.CostEstimate(
            flops=10 * rows * width * width, bytes_accessed=16 * rows * width, transcendentals=0
        ),
        name="enter_back",
    )(first, *grads, w_qk, w_vo, spread, *sources)
    return result[0], result[1:]


def norm_parts(value):
    centred = value - jnp.mean(value, axis=-1, keepdims=True)
    inverse = lax.rsqrt(jnp.mean(centred * centred, axis=-1, keepdims=True) + NORM_EPS)
    return centred * inverse, inverse


def norm_back(grad, value, gain):
    unit, inverse = norm_parts(value)
    grad_gain = jnp.sum(grad * unit, axis=0)
    grad_shift = jnp.sum(grad, axis=0)
    grad_unit = grad * gain
    grad_value = inverse * (
        grad_unit
        - jnp.mean(grad_unit, axis=-1, keepdims=True)
        - unit * jnp.mean(grad_unit * unit, axis=-1, keepdims=True)
    )
    return grad_value, grad_gain, grad_shift


class Weights:
    def __init__(self, w_qk, w_vo, spread):
        width = spread.shape[0]
        self.w_qk, self.w_vo = w_qk, w_vo
        place = w_vo[:, 2 * width :]
        self.vec_plain = jnp.transpose(project(spread, place))
        self.vec_place = jnp.transpose(place.astype(jnp.float32))
        self.w_up = self.w_down = None


def layer_ahead(rows, weights, lengths, seq, during_attend, during_expand):
    width = rows.shape[1]
    plain, vec_place = weights.vec_plain, weights.vec_place
    bias_q, bias_v, bias_up = plain[0], plain[1], plain[8:12].reshape(1, -1)
    bias_qk = jnp.concatenate([bias_q, jnp.zeros_like(bias_q)])
    qk = lowered(project(rows, weights.w_qk) + bias_qk)
    values = lowered(project(rows, weights.w_vo[:, :width]) + bias_v)
    context = during_attend(lengths, qk, values, seq)
    first_sum = (
        rows.astype(jnp.float32)
        + project_back(context, weights.w_vo[:, width : 2 * width])
        + vec_place[2]
    )
    normed = lowered(norm_parts(first_sum)[0] * vec_place[3] + vec_place[4])
    active, slope = during_expand(normed, bias_up)
    second_sum = normed.astype(jnp.float32) + project_back(active, weights.w_down) + vec_place[7]
    output = lowered(norm_parts(second_sum)[0] * vec_place[5] + vec_place[6])
    return output, (qk, values, context, first_sum, normed, active, slope, second_sum)


def layer_behind(grad_out, rows, kept, weights, spread, give, during_attend):
    w_vo = weights.w_vo
    vec_place = weights.vec_place
    width = rows.shape[1]
    qk, values, context, first_sum, normed, active, slope, second_sum = kept
    grad_second, gain_two, shift_two = norm_back(grad_out, second_sum, vec_place[5])
    grad_ffn = lowered(grad_second)
    bias_out = jnp.sum(grad_ffn.astype(jnp.float32), axis=0)
    up_grad, down_grad, bias_inner, grad_hidden = contract_plain(
        grad_ffn, normed, weights.w_down, weights.w_up, slope, active
    )
    give("up", up_grad)
    give("down", down_grad)
    grad_normed = grad_second + grad_hidden
    grad_first, gain_one, shift_one = norm_back(grad_normed, first_sum, vec_place[3])
    grad_attn = lowered(grad_first)
    bias_attn = jnp.sum(grad_attn.astype(jnp.float32), axis=0)
    give("out", lowered(outer_sum(grad_attn, context)))
    grad_context = lowered(project(grad_attn, w_vo[:, width : 2 * width]))
    grads = during_attend(qk, values, grad_context)
    grad_query, grad_keys, grad_values = grads
    bias_query = jnp.sum(grad_query.astype(jnp.float32), axis=0)
    bias_value = jnp.sum(grad_values.astype(jnp.float32), axis=0)
    give("value", lowered(outer_sum(rows, grad_values)))
    give("query", lowered(outer_sum(rows, grad_query)))
    give("key", lowered(outer_sum(rows, grad_keys)))
    plain = jnp.concatenate(
        [jnp.stack([bias_query, bias_value]), bias_inner.reshape(-1, width)], axis=0
    )
    placed = jnp.dot(plain, spread.astype(jnp.float32), precision=lax.Precision.HIGHEST)
    vec_grad = jnp.stack(
        [
            placed[0],
            placed[1],
            bias_attn,
            gain_one,
            shift_one,
            gain_two,
            shift_two,
            bias_out,
            placed[2],
            placed[3],
            placed[4],
            placed[5],
        ],
        axis=1,
    )
    return grad_first, grads, vec_grad


def contract_plain(grad_ffn, normed, w_down, w_up, slope, active):
    grad_inner = lowered(project(grad_ffn, w_down) * slope.astype(jnp.float32))
    return (
        lowered(outer_sum(normed, grad_inner)),
        lowered(outer_sum(grad_ffn, active)),
        jnp.sum(grad_inner.astype(jnp.float32), axis=0),
        project_back(grad_inner, w_up),
    )


def input_grad(grad_first, grads, weights):
    width = grad_first.shape[1]
    grad_rows = grad_first + project_back(grads[0], weights.w_qk[:, :width])
    grad_rows = grad_rows + project_back(grads[1], weights.w_qk[:, width:])
    return grad_rows + project_back(grads[2], weights.w_vo[:, :width])


ATTN_NAMES = ("query", "key", "value", "out")
FFN_NAMES = ("up", "down")
FLIPPED = ("value", "out", "down")


def behind_permuted(grad_rows, layer_inputs, kept_all, weights_all, lengths, seq, spread):
    summed, vec_all = {}, {}
    half = spread.shape[0] // 2
    for layer in reversed(range(len(kept_all))):

        def give(name, grad):
            keep, send = grad[:half].astype(jnp.float32), grad[half:]
            summed[layer, name] = scatter_rows(keep, send, name in FLIPPED, jnp.bfloat16)

        def during_attend(qk, values, grads):
            return attend_back(lengths, qk, values, grads, seq)[0]

        grad_first, grads, vec_all[layer] = layer_behind(
            grad_rows,
            layer_inputs[layer],
            kept_all[layer],
            weights_all[layer],
            spread,
            give,
            during_attend,
        )
        for group, names in (("attn", ATTN_NAMES), ("ffn", FFN_NAMES)):
            summed[layer, group] = jnp.concatenate([summed[layer, name] for name in names], axis=1)
        if layer:
            grad_rows = input_grad(grad_first, grads, weights_all[layer])
    vec_local = jnp.concatenate([vec_all[layer] for layer in sorted(vec_all)], axis=1)
    vec_sum = scatter_rows(vec_local[:half], vec_local[half:], False, jnp.float32)
    in_grad = enter_back(grad_first, grads, weights_all[0].w_qk, weights_all[0].w_vo, spread)[0]
    return in_grad, summed, vec_sum


def behind_carried(grad_rows, layer_inputs, kept_all, weights_all, lengths, seq, spread):
    width = spread.shape[0]
    layers = len(kept_all)
    products, eighths, summed, vec_all = {}, {}, {}, {}

    def plan(wanted):
        sources, arrays, places, results, names = [], [], [], [], []
        for layer, name, span in wanted:
            source = eighths[layer, name] if span == "back" else products[layer, name]
            sources.append(source)
            columns = source.shape[1]
            parts = 4 if columns > width else 2 if columns == width else 1
            arrays.append((columns, source.dtype, span, parts, int(name in FLIPPED)))
            key = (layer, name, span)
            if span != "front":
                key = (layer, "attn" if name in ATTN_NAMES else "ffn" if name in FFN_NAMES else name)
            if key not in names:
                names.append(key)
                results.append(0)
            place = names.index(key)
            places.append((place, results[place]))
            results[place] += columns
        shapes = [
            jax.ShapeDtypeStruct((width // 8, columns), jnp.bfloat16)
            if len(key) == 3
            else jax.ShapeDtypeStruct((width // 32, columns), jnp.float32)
            for key, columns in zip(names, results)
        ]

        def keep(arrived):
            for key, result in zip(names, arrived):
                (eighths if len(key) == 3 else summed)[key[:2]] = result

        return sources, Scatter(arrays, places, shapes, width), keep

    for layer in reversed(range(layers)):
        later = layer + 1 < layers

        def give(name, grad):
            products[layer, name] = grad

        def during_attend(qk, values, grads):
            wanted = [(layer, name, "front") for name in FFN_NAMES]
            if later:
                wanted = [(layer + 1, name, "back") for name in FFN_NAMES] + wanted
                wanted = [(layer + 1, name, "full") for name in ATTN_NAMES] + wanted
            sources, scatter, keep = plan(wanted)
            grads_qkv, arrived = attend_back(
                lengths, qk, values, grads, seq, sources, scatter, 16 + layer
            )
            keep(arrived)
            return grads_qkv

        grad_first, grads, vec_all[layer] = layer_behind(
            grad_rows,
            layer_inputs[layer],
            kept_all[layer],
            weights_all[layer],
            spread,
            give,
            during_attend,
        )
        if layer:
            grad_rows = input_grad(grad_first, grads, weights_all[layer])
    vec_local = jnp.concatenate([vec_all[layer] for layer in range(layers)], axis=1)
    vec_columns = vec_local.shape[1]
    products[0, "vec"] = jnp.pad(vec_local, ((0, 0), (0, 128 - vec_columns)))
    sources, scatter, keep = plan(
        [(0, name, "full") for name in ATTN_NAMES]
        + [(0, "vec", "full")]
        + [(0, name, "back") for name in FFN_NAMES]
    )
    in_grad, arrived = enter_back(
        grad_first, grads, weights_all[0].w_qk, weights_all[0].w_vo, spread, sources, scatter, 15
    )
    keep(arrived)
    return in_grad, summed, summed[0, "vec"][:, :vec_columns]


def ahead_permuted(rows, shards_all, spread, lengths, seq):
    layer_inputs, kept_all, weights_all = [], [], []
    for shards in shards_all:
        weights = Weights(gather_rows(shards[0], False), gather_rows(shards[1], True), spread)
        weights.w_up = gather_rows(shards[2], False)
        weights.w_down = gather_rows(shards[3], True)
        layer_inputs.append(rows)
        rows, kept = layer_ahead(
            rows,
            weights,
            lengths,
            seq,
            lambda *operands: attend(*operands)[0],
            lambda normed, bias, weights=weights: expand(normed, weights.w_up, bias)[:2],
        )
        kept_all.append(kept)
        weights_all.append(weights)
    return rows, layer_inputs, kept_all, weights_all


def ahead_carried(rows, shards_all, spread, lengths, seq):
    devices = lax.axis_size("dp")
    bits = bit_count(devices)
    layers = len(shards_all)

    along = 2
    last = bits - 1
    arrays = {}

    def plan(*wanted):
        wanted = [item for item in wanted if item[0] < layers]
        operands, shapes = [], []
        for layer, index, first, _, _ in wanted:
            shard = shards_all[layer][index][None]
            operands.append(arrays[layer, index] if first else shard)
            shapes.append((devices,) + shard.shape[1:])
        spans = [item[2:4] for item in wanted]
        delays = [item[4] for item in wanted]
        flips = [item[1] % 2 for item in wanted]

        def keep(results):
            for (layer, index, _, _, _), result in zip(wanted, results):
                arrays[layer, index] = result

        return operands, Gather(shapes, spans, delays, flips, bits), keep

    def flat(layer, index):
        array = arrays[layer, index]
        return array.reshape(-1, array.shape[2])

    operands, gather, keep = plan(
        (0, 0, 0, last, 0.0),
        (0, 1, 0, last, 0.0),
        (0, 2, 0, along - 1, 14.0),
        (1, 0, 0, along - 1, 14.0),
    )
    keep(gather_alone(gather, operands, 0))
    layer_inputs, kept_all, weights_all = [], [], []
    for layer in range(layers):
        weights = Weights(flat(layer, 0), flat(layer, 1), spread)

        def during_attend(lengths, qk, values, seq):
            operands, gather, keep = plan(
                (layer, 2, along, last, 0.0),
                (layer + 1, 0, along, last, 0.0),
                (layer, 3, 0, along - 1, 0.0),
                (layer + 1, 1, 0, along - 1, 0.0),
            )
            context, arrived = attend(
                lengths, qk, values, seq, operands, gather, 1 + 2 * layer
            )
            keep(arrived)
            weights.w_up = flat(layer, 2)
            return context

        def during_expand(normed, bias):
            operands, gather, keep = plan(
                (layer, 3, along, last, 0.0),
                (layer + 1, 1, along, last, 0.0),
                (layer + 1, 2, 0, along - 1, 0.0),
                (layer + 2, 0, 0, along - 1, 0.0),
            )
            active, slope, arrived = expand(
                normed, weights.w_up, bias, operands, gather, 2 + 2 * layer
            )
            keep(arrived)
            weights.w_down = flat(layer, 3)
            return active, slope

        layer_inputs.append(rows)
        rows, kept = layer_ahead(rows, weights, lengths, seq, during_attend, during_expand)
        kept_all.append(kept)
        weights_all.append(weights)
    return rows, layer_inputs, kept_all, weights_all


def adam_step(param, first, second, grad):
    first_new = 0.9 * first + 0.1 * grad
    second_new = 0.98 * second + 0.02 * grad * grad
    first_hat = first_new / (1.0 - 0.9**10)
    second_hat = second_new / (1.0 - 0.98**10)
    direction = first_hat / (jnp.sqrt(second_hat) + 1e-08) + 0.01 * param
    return (direction, first_new, second_new)


def adam_kernel(factor, *refs):
    layers = len(refs) - 7
    p_ref, m_ref, v_ref, grad_ref, step_ref, m_new_ref, v_new_ref = refs[layers:]
    for layer in range(layers):

        @pl.when(pl.program_id(0) == layer)
        def _(layer=layer):
            grad = refs[layer][...] * factor
            grad_ref[...] = grad
            step_ref[...], m_new_ref[...], v_new_ref[...] = adam_step(
                p_ref[...], m_ref[...], v_ref[...], grad
            )


def adam(grads, param, first, second, factor):
    layers, rows, columns = param.shape
    tile = columns
    whole = pl.BlockSpec((rows, tile), lambda l, j: (0, j))
    block = pl.BlockSpec((None, rows, tile), lambda l, j: (l, 0, j))
    shape = jax.ShapeDtypeStruct(param.shape, jnp.float32)
    return pl.pallas_call(
        functools.partial(adam_kernel, factor),
        grid=(layers, columns // tile),
        in_specs=[whole] * layers + [block] * 3,
        out_specs=[block] * 4,
        out_shape=[shape] * 4,
        cost_estimate=pl.CostEstimate(
            flops=20 * layers * rows * columns,
            bytes_accessed=32 * layers * rows * columns,
            transcendentals=layers * rows * columns,
        ),
        name="adam",
    )(*grads, param, first, second)


def local(
    tokens,
    cotangent,
    lengths,
    counts,
    attn_w,
    ffn_w,
    vec_w,
    attn_m,
    ffn_m,
    vec_m,
    attn_v,
    ffn_v,
    vec_v,
):
    row_total, width = tokens.shape
    seq = row_total // lengths.shape[0]
    layers = attn_w.shape[0]
    hidden = ffn_w.shape[2] // 2
    vec_rows = vec_w.shape[1]
    micro = lax.broadcasted_iota(jnp.int32, (row_total, 1), 0) // (seq * SEQ_MB)
    live = micro < counts[0]
    spread = order_matrix(width)
    shards_all = []
    for layer in range(layers):
        attn = lowered(attn_w[layer])
        ffn = lowered(ffn_w[layer])
        vec = jnp.pad(jnp.transpose(lowered(vec_w[layer])), ((0, 0), (0, 128 - vec_rows)))
        shards_all.append(
            (
                attn[:, : 2 * width],
                jnp.concatenate([attn[:, 2 * width :], vec], axis=1),
                ffn[:, :hidden],
                ffn[:, hidden:],
            )
        )
    carry = lax.axis_size("dp") == 32 and attn_w.shape[1] % 8 == 0
    ahead = ahead_carried if carry else ahead_permuted
    behind = behind_carried if carry else behind_permuted
    rows = lowered(project(tokens, spread))
    rows, layer_inputs, kept_all, weights_all = ahead(rows, shards_all, spread, lengths, seq)
    activations = lowered(jnp.where(live, project_back(rows, spread), 0.0))
    grad_rows = jnp.where(live, project(cotangent, spread), 0.0)
    in_grad, summed, vec_sum = behind(
        grad_rows, layer_inputs, kept_all, weights_all, lengths, seq, spread
    )
    vec_sum = jnp.transpose(vec_sum).reshape(layers, vec_rows, -1)
    factor = float(row_total * lax.axis_size("dp")) ** (-0.5)

    vec_grad = vec_sum * factor
    attn_grad, attn_step, attn_m_new, attn_v_new = adam(
        [summed[layer, "attn"] for layer in range(layers)], attn_w, attn_m, attn_v, factor
    )
    ffn_grad, ffn_step, ffn_m_new, ffn_v_new = adam(
        [summed[layer, "ffn"] for layer in range(layers)], ffn_w, ffn_m, ffn_v, factor
    )
    vec_step, vec_m_new, vec_v_new = adam_step(vec_w, vec_m, vec_v, vec_grad)
    return (
        activations,
        in_grad,
        attn_grad,
        ffn_grad,
        vec_grad,
        attn_step,
        ffn_step,
        vec_step,
        attn_m_new,
        ffn_m_new,
        vec_m_new,
        attn_v_new,
        ffn_v_new,
        vec_v_new,
    )


def solution(mesh):
    rows = P("dp", None)
    weight = P(None, "dp", None)
    vector = P(None, None, "dp")
    in_specs = (rows, rows, P("dp"), P("dp")) + (weight, weight, vector) * 3
    out_specs = (rows, rows) + (weight, weight, vector) * 4
    return jax.shard_map(local, mesh=mesh, in_specs=in_specs, out_specs=out_specs, check_vma=False)
```

```python
import functools

import jax
import jax.numpy as jnp
from jax import lax
from jax.experimental import pallas as pl
from jax.experimental.pallas import tpu as pltpu
from jax.sharding import PartitionSpec as P

HEAD_DIM = 64
SEQ_MB = 1
PAIR = 2 * HEAD_DIM

NORM_EPS = 1e-05
MASK_VALUE = -1e30

TAIL_P = 0.275
TAIL_C = (0.1178092576, 0.04211145346, 0.3339323636, -0.3309935012, 0.4519987806, -0.1148583494)
INV_SQRT_2PI = 0.3989422804014327


def lowered(value):
    return value.astype(jnp.bfloat16)


def project(left, right):
    return jnp.dot(left, right, preferred_element_type=jnp.float32)


def project_back(left, right):
    return lax.dot_general(
        left, right, (((1,), (1,)), ((), ())), preferred_element_type=jnp.float32
    )


def outer_sum(left, right):
    return lax.dot_general(
        left, right, (((0,), (0,)), ((), ())), preferred_element_type=jnp.float32
    )


def bit_count(devices):
    bits = devices.bit_length() - 1
    assert 1 << bits == devices
    return bits


def swap(value, bit):
    devices = lax.axis_size("dp")
    return lax.ppermute(value, "dp", [(i, i ^ (1 << bit)) for i in range(devices)])


def gather_rows(shard, flip):
    bits = bit_count(lax.axis_size("dp"))
    rows = shard
    for bit in reversed(range(3 if flip else 0, bits)):
        rows = jnp.concatenate([rows, swap(rows, bit)], axis=0)
    if flip:
        height, width = rows.shape
        rows = jnp.concatenate([rows[None], swap(rows, 1)[None]], axis=0)
        rows = jnp.concatenate([rows[:, None], swap(rows, 2)[:, None]], axis=1)
        rows = rows.reshape(4 * height, width)
        rows = jnp.concatenate([rows, swap(rows, 0)], axis=0)
    return rows


def scatter_rows(keep, send, flip, wire):
    bits = bit_count(lax.axis_size("dp"))
    total = keep + swap(send.astype(wire), 0).astype(jnp.float32)
    start = 1
    if flip:
        total = total.astype(wire)
        height, width = total.shape
        quarter = total.reshape(2, 2, height // 4, width)
        total = quarter[:, 0].astype(jnp.float32) + swap(quarter[:, 1], 2).astype(jnp.float32)
        total = total.astype(wire)
        total = total[0].astype(jnp.float32) + swap(total[1], 1).astype(jnp.float32)
        start = 3
    for bit in range(start, bits):
        total = total.astype(wire)
        half = total.shape[0] // 2
        total = total[:half].astype(jnp.float32) + swap(total[half:], bit).astype(jnp.float32)
    return total


def order_row(width):
    devices = lax.axis_size("dp")
    bits = bit_count(devices)
    block = width // devices
    place = lax.broadcasted_iota(jnp.int32, (1, width), 1)
    part = place // block
    mirrored = jnp.zeros_like(part)
    for bit in range(bits):
        mirrored = mirrored | (((part >> bit) & 1) << (bits - 1 - bit))
    return (mirrored ^ lax.axis_index("dp")) * block + place % block


def order_matrix(order):
    width = order.shape[1]
    feature = lax.broadcasted_iota(jnp.int32, (width, width), 0)
    return jnp.where(feature == order, 1.0, 0.0).astype(jnp.bfloat16)


LINK_BYTES_US = 90e3
CORE_BYTES_US = 900e3
HOP_US = 1.5
PARTS = 6
EARLY_PARTS = 2
VMEM_BYTES = 40 << 20


class Gather:
    def __init__(self, shapes, stretches, delays, flips, bits):
        self.delays = delays
        self.shapes = shapes
        self.ins = self.outs = len(shapes)
        self.stretches = stretches
        self.bits = bits
        self.pieces = []
        self.steps = []
        self.ranges = []
        for array, (shape, flip_first) in enumerate(zip(shapes, flips)):
            lanes = shape[2] // 128
            edges = [128 * (lanes * part // PARTS) for part in range(PARTS + 1)]
            for part in range(PARTS):
                near = 2 if (part + flip_first) % 2 else 1
                early = part >= PARTS - EARLY_PARTS and stretches[array] != "all"
                self.pieces.append((array, edges[part], edges[part + 1] - edges[part], early))
                self.steps.append(self.plan(near, early))
                along = bits - 3 + early
                stretch = stretches[array]
                self.ranges.append(
                    (
                        along if stretch == "second" else 0,
                        along - 1 if stretch == "first" else bits - 1,
                    )
                )
        self.slots = {}
        for piece, plan in enumerate(self.steps):
            first, last = self.ranges[piece]
            for step in range(first, last + 1):
                for run in range(len(plan[step][1])):
                    self.slots[piece, step, run] = len(self.slots)

    def plan(self, near, early):
        other = 3 - near
        order = list(reversed(range(3, self.bits)))
        order = [other] + order if early else order + [other]
        order += [near, 0]
        held = [0]
        plan = []
        for bit in order:
            offset = 1 << (self.bits - 1 - bit)
            runs = []
            for block in held:
                if runs and runs[-1][0] + runs[-1][1] == block:
                    runs[-1][1] += 1
                else:
                    runs.append([block, 1])
            plan.append((bit, [(first, count, first + offset) for first, count in runs]))
            held = sorted(held + [block + offset for block in held])
        return plan

    def timetable(self):
        free = {}
        ready = {}
        for piece, (array, _, _, early) in enumerate(self.pieces):
            ready[array, early] = (self.delays[array], array, early, self.ranges[piece][0])
        events = []
        while ready:
            time, array, early, step = min(ready.values())
            done = time
            for piece, (owner, _, columns, kind) in enumerate(self.pieces):
                if owner != array or kind != early:
                    continue
                last = self.ranges[piece][1]
                bit, runs = self.steps[piece][step]
                link = min(bit, 3)
                size = sum(count for _, count, _ in runs) * self.shapes[array][1] * columns * 2
                if bit == 0:
                    span = size / CORE_BYTES_US
                else:
                    span = size * (4 if bit == 4 else 2) / LINK_BYTES_US
                events.append((time, piece, step))
                free[link] = max(time, free.get(link, 0.0)) + span
                done = max(done, free[link])
            if step == last:
                del ready[array, early]
            else:
                ready[array, early] = (done + HOP_US, array, early, step + 1)
        return events

    def scratch(self):
        count = len(self.slots)
        return [
            pltpu.SemaphoreType.DMA((count,)),
            pltpu.SemaphoreType.DMA((count,)),
            pltpu.SemaphoreType.DMA((len(self.pieces),)),
        ]

    def in_specs(self):
        return [
            pl.BlockSpec(memory_space=pl.ANY if stretch == "second" else pltpu.VMEM)
            for stretch in self.stretches
        ]

    def out_specs(self):
        return [pl.BlockSpec(memory_space=pl.ANY)] * len(self.shapes)

    def out_shape(self):
        return [jax.ShapeDtypeStruct(shape, jnp.bfloat16) for shape in self.shapes]

    def aliases(self, inputs, outputs):
        return {
            inputs + array: outputs + array
            for array, stretch in enumerate(self.stretches)
            if stretch == "second"
        }

    def bind(self, shards, dests, sems):
        self.shards, self.dests = shards, dests
        self.send_sem, self.recv_sem, self.own_sem = sems

    def partner(self, bit):
        me = lax.axis_index("dp")
        return me + (1 << bit) * (1 - 2 * ((me // (1 << bit)) % 2))

    def copies(self, piece, step):
        array, start, columns, _ = self.pieces[piece]
        bit, runs = self.steps[piece][step]
        dest = self.dests[array]
        lanes = pl.ds(start, columns)
        made = []
        for run, (first, count, target) in enumerate(runs):
            slot = self.slots[piece, step, run]
            if step == 0:
                source = self.shards[array].at[:, :, lanes]
            else:
                source = dest.at[pl.ds(first, count), :, lanes]
            made.append(
                pltpu.make_async_remote_copy(
                    src_ref=source,
                    dst_ref=dest.at[pl.ds(target, count), :, lanes],
                    send_sem=self.send_sem.at[slot],
                    recv_sem=self.recv_sem.at[slot],
                    device_id=(self.partner(bit),),
                    device_id_type=pl.DeviceIdType.MESH,
                )
            )
        return made

    def own(self, piece):
        array, start, columns, _ = self.pieces[piece]
        lanes = pl.ds(start, columns)
        return pltpu.make_async_copy(
            self.shards[array].at[:, :, lanes],
            self.dests[array].at[pl.ds(0, 1), :, lanes],
            self.own_sem.at[piece],
        )

    def begin(self):
        barrier = pltpu.get_barrier_semaphore()
        for bit in range(self.bits):
            pl.semaphore_signal(
                barrier,
                inc=1,
                device_id=(self.partner(bit),),
                device_id_type=pl.DeviceIdType.MESH,
            )
        pl.semaphore_wait(barrier, self.bits)
        for piece in range(len(self.pieces)):
            if self.first(piece) == 0:
                self.own(piece).start()

    def first(self, piece):
        return self.ranges[piece][0]

    def last(self, piece):
        return self.ranges[piece][1]

    def advance(self, piece, step):
        if step == 1 and self.first(piece) == 0:
            self.own(piece).wait()
        if step > self.first(piece):
            for copy in self.copies(piece, step - 1):
                copy.wait_recv()
        for copy in self.copies(piece, step):
            copy.start()

    def finish(self):
        for piece in range(len(self.pieces)):
            for copy in self.copies(piece, self.last(piece)):
                copy.wait_recv()
        for piece in range(len(self.pieces)):
            for step in range(self.first(piece), self.last(piece) + 1):
                for copy in self.copies(piece, step):
                    copy.wait_send()


class Scatter:
    def __init__(self, arrays, places, results, rows):
        self.given = arrays
        self.places = places
        self.made = results
        self.rows = rows
        self.arrays = self.ins = len(arrays)
        self.outs = len(results)
        self.pieces = []
        for array, (columns, _, _, parts, first) in enumerate(arrays):
            lanes = columns // 128
            edges = [128 * (lanes * part // parts) for part in range(parts + 1)]
            for part in range(parts):
                flip = (part + first) % 2
                self.pieces.append((array, edges[part], edges[part + 1] - edges[part], flip))

    def range_of(self, array):
        return {"full": (0, 4), "front": (0, 2), "back": (3, 4)}[self.given[array][2]]

    def link(self, step, flip):
        return (0, 2, 1, 3, 4)[step] if flip else (0, 1, 2, 3, 4)[step]

    def timetable(self):
        free = {}
        ready = {array: (0.0, array, self.range_of(array)[0]) for array in range(self.arrays)}
        events = []
        while ready:
            time, array, step = min(ready.values())
            done = time
            last = self.range_of(array)[1]
            for piece, (owner, _, columns, flip) in enumerate(self.pieces):
                if owner != array:
                    continue
                events.append((time, piece, step))
                if step > last:
                    continue
                bit = self.link(step, flip)
                size = (self.rows >> (step + 1)) * columns * jnp.dtype(self.given[array][1]).itemsize
                if bit == 0:
                    span = size / CORE_BYTES_US
                else:
                    span = size * (4 if bit == 4 else 2) / LINK_BYTES_US
                link = min(bit, 3)
                free[link] = max(time, free.get(link, 0.0)) + span
                done = max(done, free[link])
            if step > last:
                del ready[array]
            else:
                ready[array] = (done + HOP_US, array, step + 1)
        return events

    def in_specs(self):
        return [
            pl.BlockSpec(memory_space=pltpu.VMEM if given[2] == "back" else pl.ANY)
            for given in self.given
        ]

    def out_specs(self):
        return [pl.BlockSpec(memory_space=pltpu.VMEM)] * self.outs

    def out_shape(self):
        return self.made

    def aliases(self, inputs, outputs):
        return {}

    def scratch(self):
        made = []
        for columns, kind, span, _, _ in self.given:
            if span != "back":
                made += [pltpu.VMEM((self.rows // 2, columns), kind)] * 2
                made.append(pltpu.VMEM((self.rows // 4, columns), kind))
                made.append(pltpu.VMEM((self.rows // 8, columns), kind))
            if span != "front":
                made.append(pltpu.VMEM((self.rows // 16, columns), kind))
                made += [pltpu.VMEM((self.rows // 32, columns), kind)] * 2
                made.append(pltpu.VMEM((self.rows // 32, columns), jnp.float32))
        count = len(self.pieces)
        made += [pltpu.SemaphoreType.DMA((count * 6,))] * 2
        made.append(pltpu.SemaphoreType.DMA((count,)))
        return made

    def bind(self, sources, results, scratch):
        self.sources, self.results = sources, results
        scratch = list(scratch)
        self.part, self.landing, self.leaving, self.own = {}, {}, {}, {}
        for array, given in enumerate(self.given):
            if given[2] != "back":
                self.part[array], self.landing[array, 0] = scratch.pop(0), scratch.pop(0)
                self.landing[array, 1], self.landing[array, 2] = scratch.pop(0), scratch.pop(0)
            else:
                self.part[array] = sources[array]
            if given[2] != "front":
                self.landing[array, 3] = scratch.pop(0)
                self.landing[array, 4], self.leaving[array] = scratch.pop(0), scratch.pop(0)
                self.own[array] = scratch.pop(0)
        self.send_sem, self.recv_sem, self.own_sem = scratch

    def partner(self, bit):
        me = lax.axis_index("dp")
        return me + (1 << bit) * (1 - 2 * ((me // (1 << bit)) % 2))

    def begin(self):
        barrier = pltpu.get_barrier_semaphore()
        for bit in range(5):
            pl.semaphore_signal(
                barrier,
                inc=1,
                device_id=(self.partner(bit),),
                device_id_type=pl.DeviceIdType.MESH,
            )
        pl.semaphore_wait(barrier, 5)

    def fetch(self, piece):
        array, start, columns, _ = self.pieces[piece]
        lanes = pl.ds(start, columns)
        half = self.rows // 2
        return pltpu.make_async_copy(
            self.sources[array].at[pl.ds(0, half), lanes],
            self.part[array].at[:, lanes],
            self.own_sem.at[piece],
        )

    def copies(self, piece, step):
        array, start, columns, flip = self.pieces[piece]
        lanes = pl.ds(start, columns)
        size = self.rows >> (step + 1)
        source = self.part[array]
        if step == 0:
            source, runs = self.sources[array], [(size, 0, size)]
        elif step == 1 and flip:
            runs = [(size // 2, 0, size // 2), (3 * size // 2, size // 2, size // 2)]
        elif step == 4:
            source, runs = self.leaving[array], [(0, 0, size)]
        elif step == 2 and flip:
            runs = [(2 * size, 0, size)]
        else:
            runs = [(size, 0, size)]
        made = []
        for run, (first, target, count) in enumerate(runs):
            slot = piece * 6 + (step if run == 0 else 5)
            made.append(
                pltpu.make_async_remote_copy(
                    src_ref=source.at[pl.ds(first, count), lanes],
                    dst_ref=self.landing[array, step].at[pl.ds(target, count), lanes],
                    send_sem=self.send_sem.at[slot],
                    recv_sem=self.recv_sem.at[slot],
                    device_id=(self.partner(self.link(step, flip)),),
                    device_id_type=pl.DeviceIdType.MESH,
                )
            )
        return made

    def add(self, piece, step):
        array, start, columns, flip = self.pieces[piece]
        lanes = pl.ds(start, columns)
        part, landed = self.part[array], self.landing[array, step]
        size = self.rows >> (step + 1)
        if step == 4:
            result, offset = self.places[array]
            self.results[result][:, pl.ds(offset + start, columns)] = self.own[array][
                :, lanes
            ] + landed[:, lanes].astype(jnp.float32)
        elif step == 3:
            total = part[pl.ds(0, size), lanes].astype(jnp.float32) + landed[:, lanes].astype(
                jnp.float32
            )
            self.own[array][:, lanes] = total[: size // 2]
            self.leaving[array][:, lanes] = total[size // 2 :].astype(self.given[array][1])
        elif step == 2 and self.given[array][2] == "front":
            result = self.places[array][0]
            self.results[result][:, lanes] = part[pl.ds(0, size), lanes] + landed[:, lanes]
        else:
            block = self.rows // 16
            skip = size // 2 if step == 1 and flip else None

            def body(index, carry):
                from_row = pl.multiple_of(index * block, block)
                row = from_row
                if skip:
                    row = pl.multiple_of(from_row + (index // (skip // block)) * skip, block)
                part[pl.ds(row, block), lanes] = (
                    part[pl.ds(row, block), lanes] + landed[pl.ds(from_row, block), lanes]
                )
                return carry

            lax.fori_loop(0, size // block, body, 0)

    def advance(self, piece, step):
        first, last = self.range_of(self.pieces[piece][0])
        if step == 0:
            self.fetch(piece).start()
        if step > first:
            if step == 1:
                self.fetch(piece).wait()
            for copy in self.copies(piece, step - 1):
                copy.wait_recv()
            self.add(piece, step - 1)
        if step <= last:
            for copy in self.copies(piece, step):
                copy.start()

    def finish(self):
        for piece in range(len(self.pieces)):
            first, last = self.range_of(self.pieces[piece][0])
            for step in range(first, last + 1):
                for copy in self.copies(piece, step):
                    copy.wait_send()


def carried(body, gather, inputs, outputs, prefetch, steps, step_us, place):
    ins, outs = gather.ins, gather.outs
    agenda = [[] for _ in range(steps)]
    for time, piece, step in gather.timetable():
        agenda[min(steps - 1, int(-(-time // step_us)))].append((piece, step))

    def kernel(*refs):
        refs = list(refs)
        cut = prefetch + inputs
        ahead, refs = refs[:cut], refs[cut:]
        shards, refs = refs[:ins], refs[ins:]
        results, refs = refs[:outputs], refs[outputs:]
        dests, sems = refs[:outs], refs[outs:]
        gather.bind(shards, dests, sems)
        here = place()
        for index, moves in enumerate(agenda):
            if index and not moves:
                continue

            @pl.when(here == index)
            def _(index=index, moves=moves):
                if index == 0:
                    gather.begin()
                for piece, step in moves:
                    gather.advance(piece, step)

        body(*ahead, *results)

        @pl.when(here == steps - 1)
        def _():
            gather.finish()

    return kernel


def head_lanes(which):
    return lax.broadcasted_iota(jnp.int32, (1, PAIR), 1) // HEAD_DIM == which


def carrier(body, exchange, inputs, outputs, prefetch, steps, step_us, place, collective):
    if exchange is None:
        return body, [], [], [], [], {}, pltpu.CompilerParams(vmem_limit_bytes=VMEM_BYTES)
    return (
        carried(body, exchange, inputs, outputs, prefetch, steps, step_us, place),
        exchange.in_specs(),
        exchange.out_specs(),
        exchange.out_shape(),
        exchange.scratch(),
        exchange.aliases(prefetch + inputs, outputs),
        pltpu.CompilerParams(
            collective_id=collective, has_side_effects=True, vmem_limit_bytes=VMEM_BYTES
        ),
    )


def enter_kernel(order_ref, tokens_ref, cotangent_ref, spread_ref, rows_ref, grads_ref):
    @pl.when(pl.program_id(0) == 0)
    def _():
        spread_ref[...] = order_matrix(order_ref[...])

    spread = spread_ref[...]
    rows_ref[...] = lowered(project(tokens_ref[...], spread))
    grads_ref[...] = lowered(project(cotangent_ref[...], spread))


def enter(order, tokens, cotangent, shards, gather, collective, tile=256):
    rows, width = tokens.shape
    body, more_in, more_out, more_shape, scratch, aliases, params = carrier(
        enter_kernel, gather, 3, 3, 0, rows // tile, 1.5, lambda: pl.program_id(0), collective
    )
    block = pl.BlockSpec((tile, width), lambda i: (i, 0))
    square = pl.BlockSpec((width, width), lambda i: (0, 0))
    shape = jax.ShapeDtypeStruct((rows, width), jnp.bfloat16)
    result = pl.pallas_call(
        body,
        grid=(rows // tile,),
        in_specs=[pl.BlockSpec((1, width), lambda i: (0, 0)), block, block] + more_in,
        out_specs=[square, block, block] + more_out,
        out_shape=[jax.ShapeDtypeStruct((width, width), jnp.bfloat16), shape, shape] + more_shape,
        scratch_shapes=scratch,
        input_output_aliases=aliases,
        compiler_params=params,
        name="enter",
    )(order, tokens, cotangent, *shards)
    return result[:3], result[3:]


def attend_kernel(len_ref, q_ref, k_ref, v_ref, ctx_ref):
    length = len_ref[pl.program_id(0)]
    seq = k_ref.shape[0]
    query = q_ref[...] * jnp.bfloat16(HEAD_DIM ** (-0.5))
    keys = k_ref[...]
    values = v_ref[...]
    open_keys = lax.broadcasted_iota(jnp.int32, (1, seq), 1) < length
    picked = []
    for which in range(2):
        lanes = head_lanes(which)
        scores = project_back(jnp.where(lanes, query, jnp.zeros_like(query)), keys)
        scores = jnp.where(open_keys, scores, MASK_VALUE)
        expo = jnp.exp(scores - jnp.max(scores, axis=-1, keepdims=True))
        chance = expo * (1.0 / jnp.sum(expo, axis=-1, keepdims=True))
        picked.append(project(lowered(chance), values))
    ctx_ref[...] = lowered(jnp.where(head_lanes(0), picked[0], picked[1]))


def attend(lengths, qk, values, seq, shards=(), gather=None, collective=None):
    rows, width = values.shape
    pairs = width // PAIR
    flops = 4 * rows * seq * width
    body, more_in, more_out, more_shape, scratch, params = attend_kernel, [], [], [], [], None
    aliases = {}
    if gather is not None:
        steps = rows // seq * pairs
        body = carried(
            attend_kernel,
            gather,
            3,
            1,
            1,
            steps,
            1.5,
            lambda: pl.program_id(0) * pairs + pl.program_id(1),
        )
        more_in, more_out, more_shape = gather.in_specs(), gather.out_specs(), gather.out_shape()
        scratch, aliases = gather.scratch(), gather.aliases(4, 1)
        params = pltpu.CompilerParams(collective_id=collective, has_side_effects=True)
    result = pl.pallas_call(
        body,
        grid_spec=pltpu.PrefetchScalarGridSpec(
            num_scalar_prefetch=1,
            grid=(rows // seq, pairs),
            in_specs=[
                pl.BlockSpec((seq, PAIR), lambda s, h, n: (s, h)),
                pl.BlockSpec((seq, PAIR), lambda s, h, n: (s, pairs + h)),
                pl.BlockSpec((seq, PAIR), lambda s, h, n: (s, h)),
            ]
            + more_in,
            out_specs=[pl.BlockSpec((seq, PAIR), lambda s, h, n: (s, h))] + more_out,
            scratch_shapes=scratch,
        ),
        out_shape=[jax.ShapeDtypeStruct((rows, width), jnp.bfloat16)] + more_shape,
        input_output_aliases=aliases,
        compiler_params=params,
        cost_estimate=pl.CostEstimate(
            flops=8 * flops, bytes_accessed=8 * rows * width, transcendentals=rows * seq * 12
        ),
        name="attend",
    )(lengths, qk, qk, values, *shards)
    return result[0], result[1:]


def attend_back_kernel(len_ref, q_ref, k_ref, v_ref, g_ref, dq_ref, dk_ref, dv_ref):
    length = len_ref[pl.program_id(0)]
    seq = k_ref.shape[0]
    query = q_ref[...] * jnp.bfloat16(HEAD_DIM ** (-0.5))
    keys = k_ref[...]
    values = v_ref[...]
    grads = g_ref[...]
    open_keys = lax.broadcasted_iota(jnp.int32, (seq, 1), 0) < length
    parts = []
    for which in range(2):
        lanes = head_lanes(which)
        scores = project_back(keys, jnp.where(lanes, query, jnp.zeros_like(query)))
        scores = jnp.where(open_keys, scores, MASK_VALUE)
        expo = jnp.exp(scores - jnp.max(scores, axis=0, keepdims=True))
        chance = expo * (1.0 / jnp.sum(expo, axis=0, keepdims=True))
        grad_chance = project_back(values, jnp.where(lanes, grads, jnp.zeros_like(grads)))
        weighed = jnp.sum(chance * grad_chance, axis=0, keepdims=True)
        grad_scores = lowered(chance * (grad_chance - weighed))
        parts.append(
            (
                outer_sum(grad_scores, keys) * HEAD_DIM ** (-0.5),
                project(grad_scores, query),
                project(lowered(chance), grads),
            )
        )
    first = head_lanes(0)
    for index, out_ref in enumerate((dq_ref, dk_ref, dv_ref)):
        out_ref[...] = lowered(jnp.where(first, parts[0][index], parts[1][index]))


def attend_back(lengths, qk, values, grads, seq, sources=(), scatter=None, collective=None):
    rows, width = values.shape
    pairs = width // PAIR
    flops = 10 * rows * seq * width
    spec = pl.BlockSpec((seq, PAIR), lambda s, h, n: (s, h))
    shape = jax.ShapeDtypeStruct((rows, width), jnp.bfloat16)
    body, more_in, more_out, more_shape, scratch, params = attend_back_kernel, [], [], [], [], None
    if scatter is not None:
        body = carried(
            attend_back_kernel,
            scatter,
            4,
            3,
            1,
            rows // seq * pairs,
            2.7,
            lambda: pl.program_id(0) * pairs + pl.program_id(1),
        )
        more_in, more_out, more_shape = scatter.in_specs(), scatter.out_specs(), scatter.out_shape()
        scratch = scatter.scratch()
        params = pltpu.CompilerParams(
            collective_id=collective, has_side_effects=True, vmem_limit_bytes=VMEM_BYTES
        )
    result = pl.pallas_call(
        body,
        grid_spec=pltpu.PrefetchScalarGridSpec(
            num_scalar_prefetch=1,
            grid=(rows // seq, pairs),
            in_specs=[
                spec,
                pl.BlockSpec((seq, PAIR), lambda s, h, n: (s, pairs + h)),
                spec,
                spec,
            ]
            + more_in,
            out_specs=[spec, spec, spec] + more_out,
            scratch_shapes=scratch,
        ),
        out_shape=[shape, shape, shape] + more_shape,
        compiler_params=params,
        cost_estimate=pl.CostEstimate(
            flops=8 * flops, bytes_accessed=14 * rows * width, transcendentals=rows * seq * 12
        ),
        name="attend_back",
    )(lengths, qk, qk, values, grads, *sources)
    return result[:3], result[3:]


def expand_kernel(h_ref, w_ref, b_ref, u_ref, slope_ref):
    inner = project(h_ref[...], w_ref[...]) + b_ref[...]
    bell = jnp.exp(inner * inner * -0.5)
    step = 1.0 / (1.0 + TAIL_P * jnp.abs(inner))
    poly = jnp.full_like(step, TAIL_C[-1])
    for coefficient in reversed(TAIL_C[:-1]):
        poly = poly * step + coefficient
    tail = poly * step * bell
    below = jnp.where(inner >= 0, 1.0 - tail, tail)
    u_ref[...] = lowered(inner * below)
    slope_ref[...] = lowered(below + inner * bell * INV_SQRT_2PI)


def expand(normed, weight, bias, shards=(), gather=None, collective=None, tile=256):
    rows, width = normed.shape
    hidden = weight.shape[1]
    body, more_in, more_out, more_shape, scratch, params = expand_kernel, [], [], [], [], None
    aliases = {}
    if gather is not None:
        body = carried(
            expand_kernel, gather, 3, 2, 0, hidden // tile, 1.6, lambda: pl.program_id(0)
        )
        more_in, more_out, more_shape = gather.in_specs(), gather.out_specs(), gather.out_shape()
        scratch, aliases = gather.scratch(), gather.aliases(3, 2)
        params = pltpu.CompilerParams(collective_id=collective, has_side_effects=True)
    shape = jax.ShapeDtypeStruct((rows, hidden), jnp.bfloat16)
    out_spec = pl.BlockSpec((rows, tile), lambda j: (0, j))
    result = pl.pallas_call(
        body,
        grid=(hidden // tile,),
        in_specs=[
            pl.BlockSpec((rows, width), lambda j: (0, 0)),
            pl.BlockSpec((width, tile), lambda j: (0, j)),
            pl.BlockSpec((1, tile), lambda j: (0, j)),
        ]
        + more_in,
        out_specs=[out_spec, out_spec] + more_out,
        out_shape=[shape, shape] + more_shape,
        scratch_shapes=scratch,
        input_output_aliases=aliases,
        compiler_params=params,
        cost_estimate=pl.CostEstimate(
            flops=6 * rows * width * hidden,
            bytes_accessed=2 * width * hidden + 4 * rows * hidden,
            transcendentals=2 * rows * hidden,
        ),
        name="expand",
    )(normed, weight, bias, *shards)
    return result[0], result[1], result[2:]


def enter_back_kernel(first_ref, dq_ref, dk_ref, dv_ref, qk_ref, vo_ref, spread_ref, out_ref):
    width = first_ref.shape[1]
    total = first_ref[...] + project_back(dq_ref[...], qk_ref[:, :width])
    total = total + project_back(dk_ref[...], qk_ref[:, width:])
    total = total + project_back(dv_ref[...], vo_ref[:, :width])
    high = lowered(total)
    rest = lowered(total - high.astype(jnp.float32))
    spread = spread_ref[...]
    out_ref[...] = project_back(high, spread) + project_back(rest, spread)


def enter_back(
    first, grads, w_qk, w_vo, spread, sources=(), scatter=None, collective=None, tile=256
):
    rows, width = first.shape
    body, more_in, more_out, more_shape, scratch, aliases, params = carrier(
        enter_back_kernel, scatter, 7, 1, 0, rows // tile, 3.9, lambda: pl.program_id(0), collective
    )
    block = pl.BlockSpec((tile, width), lambda i: (i, 0))

    def whole(shape):
        return pl.BlockSpec(shape, lambda i: (0, 0))

    result = pl.pallas_call(
        body,
        grid=(rows // tile,),
        in_specs=[
            block,
            block,
            block,
            block,
            whole(w_qk.shape),
            whole(w_vo.shape),
            whole(spread.shape),
        ]
        + more_in,
        out_specs=[block] + more_out,
        out_shape=[jax.ShapeDtypeStruct((rows, width), jnp.float32)] + more_shape,
        scratch_shapes=scratch,
        input_output_aliases=aliases,
        compiler_params=params,
        cost_estimate=pl.CostEstimate(
            flops=10 * rows * width * width, bytes_accessed=16 * rows * width, transcendentals=0
        ),
        name="enter_back",
    )(first, *grads, w_qk, w_vo, spread, *sources)
    return result[0], result[1:]


def norm_parts(value):
    centred = value - jnp.mean(value, axis=-1, keepdims=True)
    inverse = lax.rsqrt(jnp.mean(centred * centred, axis=-1, keepdims=True) + NORM_EPS)
    return centred * inverse, inverse


def norm_back(grad, value, gain):
    unit, inverse = norm_parts(value)
    grad_gain = jnp.sum(grad * unit, axis=0)
    grad_shift = jnp.sum(grad, axis=0)
    grad_unit = grad * gain
    grad_value = inverse * (
        grad_unit
        - jnp.mean(grad_unit, axis=-1, keepdims=True)
        - unit * jnp.mean(grad_unit * unit, axis=-1, keepdims=True)
    )
    return grad_value, grad_gain, grad_shift


class Weights:
    def __init__(self, w_qk, w_vo, spread):
        width = spread.shape[0]
        self.w_qk, self.w_vo = w_qk, w_vo
        place = w_vo[:, 2 * width :]
        self.vec_plain = jnp.transpose(project(spread, place))
        self.vec_place = jnp.transpose(place.astype(jnp.float32))
        self.w_up = self.w_down = None


def layer_ahead(rows, weights, lengths, seq, during_attend, during_expand):
    width = rows.shape[1]
    plain, vec_place = weights.vec_plain, weights.vec_place
    bias_q, bias_v, bias_up = plain[0], plain[1], plain[8:12].reshape(1, -1)
    bias_qk = jnp.concatenate([bias_q, jnp.zeros_like(bias_q)])
    qk = lowered(project(rows, weights.w_qk) + bias_qk)
    values = lowered(project(rows, weights.w_vo[:, :width]) + bias_v)
    context = during_attend(lengths, qk, values, seq)
    first_sum = (
        rows.astype(jnp.float32)
        + project_back(context, weights.w_vo[:, width : 2 * width])
        + vec_place[2]
    )
    normed = lowered(norm_parts(first_sum)[0] * vec_place[3] + vec_place[4])
    active, slope = during_expand(normed, bias_up)
    second_sum = normed.astype(jnp.float32) + project_back(active, weights.w_down) + vec_place[7]
    output = lowered(norm_parts(second_sum)[0] * vec_place[5] + vec_place[6])
    return output, (qk, values, context, first_sum, normed, active, slope, second_sum)


def layer_behind(grad_out, rows, kept, weights, spread, give, during_attend):
    w_vo = weights.w_vo
    vec_place = weights.vec_place
    width = rows.shape[1]
    qk, values, context, first_sum, normed, active, slope, second_sum = kept
    grad_second, gain_two, shift_two = norm_back(grad_out, second_sum, vec_place[5])
    grad_ffn = lowered(grad_second)
    bias_out = jnp.sum(grad_ffn.astype(jnp.float32), axis=0)
    up_grad, down_grad, bias_inner, grad_hidden = contract_plain(
        grad_ffn, normed, weights.w_down, weights.w_up, slope, active
    )
    give("up", up_grad)
    give("down", down_grad)
    grad_normed = grad_second + grad_hidden
    grad_first, gain_one, shift_one = norm_back(grad_normed, first_sum, vec_place[3])
    grad_attn = lowered(grad_first)
    bias_attn = jnp.sum(grad_attn.astype(jnp.float32), axis=0)
    give("out", lowered(outer_sum(grad_attn, context)))
    grad_context = lowered(project(grad_attn, w_vo[:, width : 2 * width]))
    grads = during_attend(qk, values, grad_context)
    grad_query, grad_keys, grad_values = grads
    bias_query = jnp.sum(grad_query.astype(jnp.float32), axis=0)
    bias_value = jnp.sum(grad_values.astype(jnp.float32), axis=0)
    give("value", lowered(outer_sum(rows, grad_values)))
    give("query", lowered(outer_sum(rows, grad_query)))
    give("key", lowered(outer_sum(rows, grad_keys)))
    plain = jnp.concatenate(
        [jnp.stack([bias_query, bias_value]), bias_inner.reshape(-1, width)], axis=0
    )
    placed = jnp.dot(plain, spread.astype(jnp.float32), precision=lax.Precision.HIGHEST)
    vec_grad = jnp.stack(
        [
            placed[0],
            placed[1],
            bias_attn,
            gain_one,
            shift_one,
            gain_two,
            shift_two,
            bias_out,
            placed[2],
            placed[3],
            placed[4],
            placed[5],
        ],
        axis=1,
    )
    return grad_first, grads, vec_grad


def contract_plain(grad_ffn, normed, w_down, w_up, slope, active):
    grad_inner = lowered(project(grad_ffn, w_down) * slope.astype(jnp.float32))
    return (
        lowered(outer_sum(normed, grad_inner)),
        lowered(outer_sum(grad_ffn, active)),
        jnp.sum(grad_inner.astype(jnp.float32), axis=0),
        project_back(grad_inner, w_up),
    )


def input_grad(grad_first, grads, weights):
    width = grad_first.shape[1]
    grad_rows = grad_first + project_back(grads[0], weights.w_qk[:, :width])
    grad_rows = grad_rows + project_back(grads[1], weights.w_qk[:, width:])
    return grad_rows + project_back(grads[2], weights.w_vo[:, :width])


ATTN_NAMES = ("query", "key", "value", "out")
FFN_NAMES = ("up", "down")
FLIPPED = ("value", "out", "down")


def behind_permuted(grad_rows, layer_inputs, kept_all, weights_all, lengths, seq, spread):
    summed, vec_all = {}, {}
    half = spread.shape[0] // 2
    for layer in reversed(range(len(kept_all))):

        def give(name, grad):
            keep, send = grad[:half].astype(jnp.float32), grad[half:]
            summed[layer, name] = scatter_rows(keep, send, name in FLIPPED, jnp.bfloat16)

        def during_attend(qk, values, grads):
            return attend_back(lengths, qk, values, grads, seq)[0]

        grad_first, grads, vec_all[layer] = layer_behind(
            grad_rows,
            layer_inputs[layer],
            kept_all[layer],
            weights_all[layer],
            spread,
            give,
            during_attend,
        )
        for group, names in (("attn", ATTN_NAMES), ("ffn", FFN_NAMES)):
            summed[layer, group] = jnp.concatenate([summed[layer, name] for name in names], axis=1)
        if layer:
            grad_rows = input_grad(grad_first, grads, weights_all[layer])
    vec_local = jnp.concatenate([vec_all[layer] for layer in sorted(vec_all)], axis=1)
    vec_sum = scatter_rows(vec_local[:half], vec_local[half:], False, jnp.float32)
    in_grad = enter_back(grad_first, grads, weights_all[0].w_qk, weights_all[0].w_vo, spread)[0]
    return in_grad, summed, vec_sum


def behind_carried(grad_rows, layer_inputs, kept_all, weights_all, lengths, seq, spread):
    width = spread.shape[0]
    layers = len(kept_all)
    products, eighths, summed, vec_all = {}, {}, {}, {}

    def plan(wanted):
        sources, arrays, places, results, names = [], [], [], [], []
        for layer, name, span in wanted:
            source = eighths[layer, name] if span == "back" else products[layer, name]
            sources.append(source)
            columns = source.shape[1]
            parts = 4 if columns > width else 2 if columns == width else 1
            arrays.append((columns, source.dtype, span, parts, int(name in FLIPPED)))
            key = (layer, name, span)
            if span != "front":
                key = (layer, "attn" if name in ATTN_NAMES else "ffn" if name in FFN_NAMES else name)
            if key not in names:
                names.append(key)
                results.append(0)
            place = names.index(key)
            places.append((place, results[place]))
            results[place] += columns
        shapes = [
            jax.ShapeDtypeStruct((width // 8, columns), jnp.bfloat16)
            if len(key) == 3
            else jax.ShapeDtypeStruct((width // 32, columns), jnp.float32)
            for key, columns in zip(names, results)
        ]

        def keep(arrived):
            for key, result in zip(names, arrived):
                (eighths if len(key) == 3 else summed)[key[:2]] = result

        return sources, Scatter(arrays, places, shapes, width), keep

    for layer in reversed(range(layers)):
        later = layer + 1 < layers

        def give(name, grad):
            products[layer, name] = grad

        def during_attend(qk, values, grads):
            wanted = [(layer, name, "front") for name in FFN_NAMES]
            if later:
                wanted = [(layer + 1, name, "back") for name in FFN_NAMES] + wanted
                wanted = [(layer + 1, name, "full") for name in ATTN_NAMES] + wanted
            sources, scatter, keep = plan(wanted)
            grads_qkv, arrived = attend_back(
                lengths, qk, values, grads, seq, sources, scatter, 16 + layer
            )
            keep(arrived)
            return grads_qkv

        grad_first, grads, vec_all[layer] = layer_behind(
            grad_rows,
            layer_inputs[layer],
            kept_all[layer],
            weights_all[layer],
            spread,
            give,
            during_attend,
        )
        if layer:
            grad_rows = input_grad(grad_first, grads, weights_all[layer])
    vec_local = jnp.concatenate([vec_all[layer] for layer in range(layers)], axis=1)
    vec_columns = vec_local.shape[1]
    products[0, "vec"] = jnp.pad(vec_local, ((0, 0), (0, 128 - vec_columns)))
    sources, scatter, keep = plan(
        [(0, name, "full") for name in ATTN_NAMES]
        + [(0, "vec", "full")]
        + [(0, name, "back") for name in FFN_NAMES]
    )
    in_grad, arrived = enter_back(
        grad_first, grads, weights_all[0].w_qk, weights_all[0].w_vo, spread, sources, scatter, 15
    )
    keep(arrived)
    return in_grad, summed, summed[0, "vec"][:, :vec_columns]


def ahead_permuted(tokens, cotangent, shards_all, order, lengths, seq):
    spread = order_matrix(order)
    rows, grads = lowered(project(tokens, spread)), lowered(project(cotangent, spread))
    layer_inputs, kept_all, weights_all = [], [], []
    for shards in shards_all:
        weights = Weights(gather_rows(shards[0], False), gather_rows(shards[1], True), spread)
        weights.w_up = gather_rows(shards[2], False)
        weights.w_down = gather_rows(shards[3], True)
        layer_inputs.append(rows)
        rows, kept = layer_ahead(
            rows,
            weights,
            lengths,
            seq,
            lambda *operands: attend(*operands)[0],
            lambda normed, bias, weights=weights: expand(normed, weights.w_up, bias)[:2],
        )
        kept_all.append(kept)
        weights_all.append(weights)
    return rows, grads, spread, layer_inputs, kept_all, weights_all


def ahead_carried(tokens, cotangent, shards_all, order, lengths, seq):
    devices = lax.axis_size("dp")
    bits = bit_count(devices)
    layers = len(shards_all)

    arrays = {}

    def plan(*wanted):
        wanted = [item for item in wanted if item[0] < layers]
        operands, shapes = [], []
        for layer, index, stretch, _ in wanted:
            shard = shards_all[layer][index][None]
            operands.append(arrays[layer, index] if stretch == "second" else shard)
            shapes.append((devices,) + shard.shape[1:])
        stretches = [item[2] for item in wanted]
        delays = [item[3] for item in wanted]
        flips = [item[1] % 2 for item in wanted]

        def keep(results):
            for (layer, index, _, _), result in zip(wanted, results):
                arrays[layer, index] = result

        return operands, Gather(shapes, stretches, delays, flips, bits), keep

    def flat(layer, index):
        array = arrays[layer, index]
        return array.reshape(-1, array.shape[2])

    operands, gather, keep = plan(
        (0, 0, "all", 0.0),
        (0, 1, "all", 0.0),
        (0, 2, "first", 14.0),
        (1, 0, "first", 14.0),
    )
    (spread, rows, grads), arrived = enter(order, tokens, cotangent, operands, gather, 0)
    keep(arrived)
    layer_inputs, kept_all, weights_all = [], [], []
    for layer in range(layers):
        weights = Weights(flat(layer, 0), flat(layer, 1), spread)

        def during_attend(lengths, qk, values, seq):
            operands, gather, keep = plan(
                (layer, 2, "second", 0.0),
                (layer + 1, 0, "second", 0.0),
                (layer, 3, "first", 0.0),
                (layer + 1, 1, "first", 0.0),
            )
            context, arrived = attend(
                lengths, qk, values, seq, operands, gather, 1 + 2 * layer
            )
            keep(arrived)
            weights.w_up = flat(layer, 2)
            return context

        def during_expand(normed, bias):
            operands, gather, keep = plan(
                (layer, 3, "second", 0.0),
                (layer + 1, 1, "second", 0.0),
                (layer + 1, 2, "first", 0.0),
                (layer + 2, 0, "first", 0.0),
            )
            active, slope, arrived = expand(
                normed, weights.w_up, bias, operands, gather, 2 + 2 * layer
            )
            keep(arrived)
            weights.w_down = flat(layer, 3)
            return active, slope

        layer_inputs.append(rows)
        rows, kept = layer_ahead(rows, weights, lengths, seq, during_attend, during_expand)
        kept_all.append(kept)
        weights_all.append(weights)
    return rows, grads, spread, layer_inputs, kept_all, weights_all


def adam_step(param, first, second, grad):
    first_new = 0.9 * first + 0.1 * grad
    second_new = 0.98 * second + 0.02 * grad * grad
    first_hat = first_new / (1.0 - 0.9**10)
    second_hat = second_new / (1.0 - 0.98**10)
    direction = first_hat / (jnp.sqrt(second_hat) + 1e-08) + 0.01 * param
    return (direction, first_new, second_new)


def adam_kernel(factor, *refs):
    layers = len(refs) - 7
    p_ref, m_ref, v_ref, grad_ref, step_ref, m_new_ref, v_new_ref = refs[layers:]
    for layer in range(layers):

        @pl.when(pl.program_id(0) == layer)
        def _(layer=layer):
            grad = refs[layer][...] * factor
            grad_ref[...] = grad
            step_ref[...], m_new_ref[...], v_new_ref[...] = adam_step(
                p_ref[...], m_ref[...], v_ref[...], grad
            )


def adam(grads, param, first, second, factor):
    layers, rows, columns = param.shape
    tile = columns
    whole = pl.BlockSpec((rows, tile), lambda l, j: (0, j))
    block = pl.BlockSpec((None, rows, tile), lambda l, j: (l, 0, j))
    shape = jax.ShapeDtypeStruct(param.shape, jnp.float32)
    return pl.pallas_call(
        functools.partial(adam_kernel, factor),
        grid=(layers, columns // tile),
        in_specs=[whole] * layers + [block] * 3,
        out_specs=[block] * 4,
        out_shape=[shape] * 4,
        cost_estimate=pl.CostEstimate(
            flops=20 * layers * rows * columns,
            bytes_accessed=32 * layers * rows * columns,
            transcendentals=layers * rows * columns,
        ),
        name="adam",
    )(*grads, param, first, second)


def local(
    tokens,
    cotangent,
    lengths,
    counts,
    attn_w,
    ffn_w,
    vec_w,
    attn_m,
    ffn_m,
    vec_m,
    attn_v,
    ffn_v,
    vec_v,
):
    row_total, width = tokens.shape
    seq = row_total // lengths.shape[0]
    layers = attn_w.shape[0]
    hidden = ffn_w.shape[2] // 2
    vec_rows = vec_w.shape[1]
    micro = lax.broadcasted_iota(jnp.int32, (row_total, 1), 0) // (seq * SEQ_MB)
    live = micro < counts[0]
    order = order_row(width)
    shards_all = []
    for layer in range(layers):
        attn = lowered(attn_w[layer])
        ffn = lowered(ffn_w[layer])
        vec = jnp.pad(jnp.transpose(lowered(vec_w[layer])), ((0, 0), (0, 128 - vec_rows)))
        shards_all.append(
            (
                attn[:, : 2 * width],
                jnp.concatenate([attn[:, 2 * width :], vec], axis=1),
                ffn[:, :hidden],
                ffn[:, hidden:],
            )
        )
    carry = lax.axis_size("dp") == 32 and attn_w.shape[1] % 8 == 0
    ahead = ahead_carried if carry else ahead_permuted
    behind = behind_carried if carry else behind_permuted
    rows, grads, spread, layer_inputs, kept_all, weights_all = ahead(
        tokens, cotangent, shards_all, order, lengths, seq
    )
    activations = lowered(jnp.where(live, project_back(rows, spread), 0.0))
    grad_rows = jnp.where(live, grads.astype(jnp.float32), 0.0)
    in_grad, summed, vec_sum = behind(
        grad_rows, layer_inputs, kept_all, weights_all, lengths, seq, spread
    )
    vec_sum = jnp.transpose(vec_sum).reshape(layers, vec_rows, -1)
    factor = float(row_total * lax.axis_size("dp")) ** (-0.5)

    vec_grad = vec_sum * factor
    attn_grad, attn_step, attn_m_new, attn_v_new = adam(
        [summed[layer, "attn"] for layer in range(layers)], attn_w, attn_m, attn_v, factor
    )
    ffn_grad, ffn_step, ffn_m_new, ffn_v_new = adam(
        [summed[layer, "ffn"] for layer in range(layers)], ffn_w, ffn_m, ffn_v, factor
    )
    vec_step, vec_m_new, vec_v_new = adam_step(vec_w, vec_m, vec_v, vec_grad)
    return (
        activations,
        in_grad,
        attn_grad,
        ffn_grad,
        vec_grad,
        attn_step,
        ffn_step,
        vec_step,
        attn_m_new,
        ffn_m_new,
        vec_m_new,
        attn_v_new,
        ffn_v_new,
        vec_v_new,
    )


def solution(mesh):
    rows = P("dp", None)
    weight = P(None, "dp", None)
    vector = P(None, None, "dp")
    in_specs = (rows, rows, P("dp"), P("dp")) + (weight, weight, vector) * 3
    out_specs = (rows, rows) + (weight, weight, vector) * 4
    return jax.shard_map(local, mesh=mesh, in_specs=in_specs, out_specs=out_specs, check_vma=False)
```
